512 devices in a mesh: src: 8 (over x, core), tgt: 64 (over y, z).
Axes of the slice: x: 4, y: 4, z: 16, core: 2. Of those that a mesh axis runs over, the one named last changes fastest.
Arguments:
- source_points: float32 [32, 16384], P(None, ('src', 'tgt')), may hold values from -1.25 to 1.25
- target_points: float32 [32, 65536], P('src', 'tgt'), may hold values from -1.2 to 1.2
- source_potential: float32 [16384], P(('src', 'tgt')), may hold values from -1.5 to 1.5
- target_potential: float32 [65536], P('tgt'), may hold values from -1.5 to 1.5
- source_weight: float32 [16384], P(('src', 'tgt')), may hold values from 0.5 to 2
- target_weight: float32 [65536], P('tgt'), may hold values from 0.5 to 2
- core_previous: float32 [34, 34], replicated, may hold values from -0.12 to 0.12
Outputs:
- source_new: float32 [16384], P(('src', 'tgt'))
- target_new: float32 [65536], P('tgt')
- core_new: float32 [34, 34], replicated
The draws below stay inside these ranges and needn't reach their ends.
All inputs are finite; a program needn't handle non-finite values.
Results may differ from the reference program's by a relative error of at most 0.0002.
Values sent between devices are 32-bit elements; how exact they have to be, the bound alone decides.
No kernel may reach another device: no remote copies, remote signals or barrier semaphores. Data moves between devices by JAX's collectives and lax.ppermute only.
A program may use at most 64 MiB of HBM per device.

```python
import math
import jax
import jax.numpy as jnp
from jax import lax

EMB = 32
RANK = 34
SOURCES = 16384
TARGETS = 65536


def draw_source_points(key, part):
    shape = (EMB, SOURCES)
    return jnp.clip(0.18 * jax.random.normal(key, shape, jnp.float32), -1.2, 1.2)


def draw_target_points(key, part):
    shape = (EMB, TARGETS)
    local_key = jax.random.fold_in(key, 23)
    return jnp.clip(0.18 * jax.random.normal(local_key, shape, jnp.float32), -1.2, 1.2)


def draw_core_previous(key, part):
    shape = (RANK, RANK)
    local_key = jax.random.fold_in(key, 37)
    return jnp.clip(0.02 * jax.random.normal(local_key, shape, jnp.float32), -0.12, 0.12)


def block_levels(key, extent, pieces, least, top_value):
    def one(dim, shards_of):
        heights = jax.random.uniform(jax.random.fold_in(jax.random.fold_in(key, 6), dim), (shards_of,), jnp.float32, least / len(pieces), top_value / len(pieces))
        return jnp.repeat(jnp.exp(heights), extent[dim] // shards_of).reshape((-1,) + (1,) * (len(extent) - dim - 1))

    gain = one(*pieces[0])
    for cut in pieces[1:]:
        gain = gain * one(*cut)
    return gain


def normal_values(key, extent, spread, most, pieces=(), held_as=jnp.bfloat16):
    level = block_levels(key, extent, pieces, -0.22, 0.18) if pieces else 1.0
    values = jax.random.normal(key, extent, jnp.float32) * spread * level
    return jnp.minimum(jnp.maximum(values, -most), most).astype(held_as)


def setup_inputs(seed: int = 0) -> dict:
    seeds = jax.random.split(jax.random.key(seed), 8)
    return {
        "source_points": draw_source_points(jax.random.fold_in(seeds[7], 71), 0),
        "target_points": draw_target_points(jax.random.fold_in(seeds[7], 71), 0),
        "source_potential": normal_values(seeds[2], (SOURCES,), 0.25, 1.5, ((0, 512),), jnp.float32),
        "target_potential": normal_values(seeds[3], (TARGETS,), 0.25, 1.5, ((0, 64),), jnp.float32),
        "source_weight": jnp.clip(jnp.exp(math.log(2.0) - 1.3862944 * jax.random.uniform(seeds[4], (SOURCES,), jnp.float32) ** block_levels(seeds[4], (SOURCES,), ((0, 512),), -0.2, 0.2)), 0.5, 2.0),
        "target_weight": jnp.clip(jnp.exp(math.log(2.0) - 1.3862944 * jax.random.uniform(seeds[5], (TARGETS,), jnp.float32) ** block_levels(seeds[5], (TARGETS,), ((0, 64),), -0.2, 0.2)), 0.5, 2.0),
        "core_previous": draw_core_previous(jax.random.fold_in(seeds[7], 71), 0),
    }


EPSILON = 0.5
HIGHEST = lax.Precision.HIGHEST


def factors(points):
    squares = jnp.sum(points * points, axis=0, keepdims=True)
    unit_row = jnp.ones_like(squares)
    return jnp.concatenate([squares, unit_row, -2.0 * points], 0), jnp.concatenate([unit_row, squares, points], 0)


def contract_rank(left_block, weighted):
    return lax.dot_general(left_block, weighted, (((0,), (0,)), ((), ())), precision=HIGHEST, preferred_element_type=jnp.float32)


def contract_last(former, latter):
    return lax.dot_general(former, latter, (((1,), (1,)), ((), ())), precision=HIGHEST, preferred_element_type=jnp.float32)


def row_blocks(values, block_size):
    number = values.shape[-1] // block_size
    shaped = values.reshape(values.shape[:-1] + (number, block_size))
    return jnp.moveaxis(shaped, -2, 0)


def reference(source_points, target_points, source_potential, target_potential, source_weight, target_weight, core_previous):
    log_source = jnp.log(source_weight) - jnp.log(jnp.float32(SOURCES))
    log_target = jnp.log(target_weight) - jnp.log(jnp.float32(TARGETS))
    left_source, right_source = factors(source_points)
    left_target, right_target = factors(target_points)
    block_size = min(512, SOURCES)
    left_blocks = row_blocks(left_source, block_size)
    right_blocks = row_blocks(right_source, block_size)
    potential_blocks = row_blocks(source_potential, block_size)
    weight_blocks = row_blocks(log_source, block_size)
    previous_w = jnp.dot(core_previous, left_target, precision=HIGHEST)

    def plan_step(running, portion):
        left_block, right_block, potential, log_weight = portion
        scores = contract_rank(left_block, previous_w)
        plan_tile = jnp.exp(log_weight[:, None] + log_target[None, :] + (potential[:, None] + target_potential[None, :] + 2.0 * scores) / EPSILON)
        carried = contract_last(right_target, plan_tile)
        return running + contract_last(right_block, carried), None

    core_new, _ = lax.scan(plan_step, jnp.zeros((RANK, RANK), jnp.float32), (left_blocks, right_blocks, potential_blocks, weight_blocks))
    current = jnp.dot(core_new, left_target, precision=HIGHEST)

    def row_step(portion):
        left_block, log_weight = portion
        scores = log_target[None, :] + (target_potential[None, :] + 2.0 * contract_rank(left_block, current)) / EPSILON
        maxima = jnp.max(scores, axis=1)
        totals = jnp.sum(jnp.exp(scores - maxima[:, None]), axis=1)
        return EPSILON * (log_weight - maxima - jnp.log(totals))

    source_new = lax.map(row_step, (left_blocks, weight_blocks)).reshape(SOURCES)
    new_blocks = row_blocks(source_new, block_size)

    def column_step(state, portion):
        maxima, totals = state
        left_block, log_weight, potential = portion
        scores = log_weight[:, None] + (potential[:, None] + 2.0 * contract_rank(left_block, current)) / EPSILON
        highest = jnp.maximum(maxima, jnp.max(scores, axis=0))
        totals = totals * jnp.exp(maxima - highest) + jnp.sum(jnp.exp(scores - highest[None, :]), axis=0)
        return (highest, totals), None

    start = (jnp.full((TARGETS,), -jnp.inf, jnp.float32), jnp.zeros((TARGETS,), jnp.float32))
    (maxima, totals), _ = lax.scan(column_step, start, (left_blocks, weight_blocks, new_blocks))
    target_new = EPSILON * (log_target - maxima - jnp.log(totals))
    return source_new, target_new, core_new
```

```python
import math

import jax
import jax.numpy as jnp
from jax import lax
from jax.sharding import Mesh
from jax.sharding import PartitionSpec as P

PLANE = ("x", "core", "y")
ALL = ("x", "core", "y", "z")
EPSILON = 0.5
HIGHEST = lax.Precision.HIGHEST


def to_all(flat, axis):
    copies = jnp.broadcast_to(flat, (lax.axis_size(axis), 1, flat.size))
    return lax.all_to_all(copies, axis, split_axis=0, concat_axis=0, tiled=True)


def factors(points):
    squares = jnp.sum(points * points, axis=0, keepdims=True)
    unit_row = jnp.ones_like(squares)
    return (
        jnp.concatenate([squares, unit_row, -2.0 * points], 0),
        jnp.concatenate([unit_row, squares, points], 0),
    )


def contract(former, latter, dims):
    return lax.dot_general(
        former, latter, (dims, ((), ())), precision=HIGHEST, preferred_element_type=jnp.float32
    )


def logsumexp(parts, axis):
    highest = jnp.max(parts, axis=axis, keepdims=True)
    total = jnp.sum(jnp.exp(parts - highest), axis=axis)
    return jnp.squeeze(highest, axis) + jnp.log(total)


def on_device(
    source_points,
    target_points,
    source_potential,
    target_potential,
    source_weight,
    target_weight,
    core_previous,
):
    emb, own = source_points.shape
    dims, span = target_points.shape
    n_z, n_y, n_src = lax.axis_size("z"), lax.axis_size("y"), lax.axis_size(("x", "core"))
    log_sources = math.log(own * n_z * n_y * n_src)
    log_targets = math.log(span * n_z * n_y)
    src = lax.axis_index(("x", "core"))
    z = lax.axis_index("z")
    share = span // n_src

    mine = jnp.concatenate(
        [source_points.reshape(-1), source_potential, source_weight, jnp.zeros((64,), jnp.float32)]
    )
    rows = to_all(mine, "z")
    rows = rows.reshape(n_z, -1)
    points = jnp.moveaxis(rows[:, : emb * own].reshape(n_z, emb, own), 0, 1).reshape(emb, -1)
    potential = rows[:, emb * own : emb * own + own].reshape(-1)
    weight = rows[:, emb * own + own : emb * own + 2 * own].reshape(-1)

    part = lambda a: lax.dynamic_slice_in_dim(a, src * share, share)
    theirs = jnp.concatenate(
        [target_points.reshape(-1), part(target_potential), part(target_weight)]
    )
    columns = to_all(theirs, PLANE)
    columns = columns.reshape(n_src, n_y, -1)
    features = jnp.moveaxis(
        columns[:, :, : dims * span].reshape(n_src, n_y, dims, span), 1, 2
    ).reshape(emb, -1)
    offsets = jnp.moveaxis(columns[:, :, dims * span : dims * span + share], 0, 1).reshape(-1)
    masses = jnp.moveaxis(columns[:, :, dims * span + share :], 0, 1).reshape(-1)

    log_source = jnp.log(weight) - jnp.float32(log_sources)
    log_target = jnp.log(masses) - jnp.float32(log_targets)
    left_source, right_source = factors(points)
    left_target, right_target = factors(features)

    weighted = contract(core_previous, left_source, ((0,), (0,)))
    scores = contract(left_target, weighted, ((0,), (0,)))
    plan = jnp.exp(
        log_source[None, :]
        + log_target[:, None]
        + (potential[None, :] + offsets[:, None] + 2.0 * scores) / EPSILON
    )
    carried = contract(right_source, plan, ((1,), (1,)))
    partial = contract(carried, right_target, ((1,), (1,)))
    rank = partial.shape[0]
    flat = jnp.pad(partial.reshape(-1), (0, -rank * rank % 128))
    flat = jnp.sum(to_all(flat, PLANE), axis=0).reshape(-1)
    flat = jnp.sum(to_all(flat, "z"), axis=0).reshape(-1)
    core_new = flat[: rank * rank].reshape(rank, rank)

    weighted = contract(core_new, left_source, ((0,), (0,)))
    cross = contract(left_target, weighted, ((0,), (0,)))
    row_parts = logsumexp(log_target[:, None] + (offsets[:, None] + 2.0 * cross) / EPSILON, 0)
    row_parts = to_all(row_parts, "z").reshape(n_z, -1)
    source_new = EPSILON * (log_source - logsumexp(row_parts, 0))
    own_rows = lax.dynamic_slice_in_dim(source_new, z * own, own)

    column_parts = logsumexp(log_source[None, :] + (source_new[None, :] + 2.0 * cross) / EPSILON, 1)
    pieces = column_parts.reshape(1, n_y, 1, span)
    pieces = jnp.broadcast_to(pieces, (n_src, n_y, 1, span)).reshape(-1, 1, span)
    pieces = lax.all_to_all(pieces, PLANE, split_axis=0, concat_axis=0, tiled=True)
    log_own = jnp.log(target_weight) - jnp.float32(log_targets)
    target_new = EPSILON * (log_own - logsumexp(pieces.reshape(-1, span), 0))
    return (own_rows, target_new, core_new)


def solution(mesh):
    finer = Mesh(mesh.devices.reshape(4, 2, 4, 16), ALL)
    source, target = P(ALL), P(("y", "z"))
    placed = (
        P(None, ALL),
        P(("x", "core"), ("y", "z")),
        source,
        target,
        source,
        target,
        P(),
    )
    return jax.shard_map(
        on_device, mesh=finer, in_specs=placed, out_specs=(source, target, P()), check_vma=False
    )
```

```python
import math

import jax
import jax.numpy as jnp
from jax import lax
from jax.experimental import pallas as pl
from jax.experimental.pallas import tpu as pltpu
from jax.sharding import Mesh
from jax.sharding import PartitionSpec as P

PLANE = ("x", "core", "y")
ALL = ("x", "core", "y", "z")
EPSILON = 0.5
HIGHEST = lax.Precision.HIGHEST
LANES = 128
PAD = 40
DEPTH = 256
LOG2E = math.log2(math.e)
LN2 = math.log(2.0)
F32, BF16 = jnp.float32, jnp.bfloat16
VMEM = pl.BlockSpec(memory_space=pltpu.VMEM)
SMEM = pl.BlockSpec(memory_space=pltpu.SMEM)


def call(body, outs, n_smem, args, scratch=(), name=None):
    specs = [SMEM] * n_smem + [VMEM] * (len(args) - n_smem)
    return pl.pallas_call(
        body,
        out_shape=tuple(jax.ShapeDtypeStruct(s, d) for s, d in outs),
        in_specs=specs,
        out_specs=tuple(VMEM for _ in outs),
        scratch_shapes=list(scratch),
        compiler_params=pltpu.CompilerParams(vmem_limit_bytes=48 * 2**20),
        name=name,
    )(*args)


def exchange(copies, axis):
    return lax.all_to_all(copies, axis, split_axis=0, concat_axis=0, tiled=True)


def dot(former, latter, dims, precision=None):
    return lax.dot_general(
        former, latter, (dims, ((), ())), precision=precision, preferred_element_type=F32
    )


def split(value):
    first = value.astype(BF16).astype(F32)
    rest = value - first
    second = rest.astype(BF16).astype(F32)
    return first, second, rest - second


def stacked(pieces, order):
    blocks = [pieces[k] for k in order]
    filler = jnp.zeros((DEPTH - PAD * len(order), pieces[0].shape[1]), F32)
    return jnp.concatenate([*blocks, filler], 0).astype(BF16)


LATTER_ORDER = (0, 0, 1, 0, 2, 1)
FORMER_ORDER = (0, 1, 0, 2, 0, 1)


def pack_rows(points, potential, weight, out):
    value = points[...]
    block = jnp.concatenate([value[8 * k : 8 * k + 8] for k in range(4)], axis=1)
    last = jnp.concatenate(
        [potential[...], weight[...], jnp.ones((1, LANES - 64), F32)], axis=1
    )
    both = jnp.concatenate([block, last], 0)
    for k in range(out.shape[0] // 9):
        out[9 * k : 9 * k + 9, :] = both


def pack_columns(where, points, potential, weight, out, held):
    for r in range(4):
        for k in range(8):
            held[8 * r + k : 8 * r + k + 1, :] = points[r : r + 1, LANES * k : LANES * k + LANES]
    src = where[0]
    held[32:33, :] = potential[pl.ds(src, 1), :]
    held[33:34, :] = weight[pl.ds(src, 1), :]
    both = held[0:34, :]
    for k in range(out.shape[0] // 34):
        out[34 * k : 34 * k + 34, :] = both


def column_stack(log_targets):
    def body(message, out):
        for y in range(4):
            for k in range(8):
                points = jnp.concatenate(
                    [message[pl.ds(34 * (4 * s + y) + k, 4, stride=8), :] for s in range(8)], 0
                )
                squares = jnp.sum(points * points, 0, keepdims=True)
                at = 34 * (4 * k + y) + 32
                offset = jnp.log(message[at + 1 : at + 2, :]) - log_targets
                offset = (offset + message[at : at + 1, :] * (1.0 / EPSILON)) * LOG2E
                tail = jnp.concatenate(
                    [squares, jnp.ones((1, LANES), F32), offset, jnp.zeros((5, LANES), F32)], 0
                )
                value = jnp.concatenate([points, tail], 0)
                col = 1024 * y + LANES * k
                out[:, col : col + LANES] = stacked(split(value), LATTER_ORDER)

    return body


def signs(core):
    row = lax.broadcasted_iota(jnp.int32, core.shape, 0)
    col = lax.broadcasted_iota(jnp.int32, core.shape, 1)
    core = jnp.where(row < 32, -2.0 * core, core)
    return jnp.where(col < 32, -2.0 * core, core)


def former_stack(core, features, row_term, column_factor):
    weighted = dot(signs(core), features, ((0,), (0,)), HIGHEST) * (2.0 / EPSILON * LOG2E)
    row = lax.broadcasted_iota(jnp.int32, weighted.shape, 0)
    if row_term is not None:
        weighted = jnp.where(row == 33, weighted + row_term * LOG2E, weighted)
    weighted = jnp.where(row == 34, column_factor, weighted)
    return stacked(split(weighted), FORMER_ORDER)


def core_kernel(log_sources, blocks):
    def body(message, columns, core, packed, features_out, log_out, former, total):
        pieces = []
        for k in range(4):
            pieces.append(
                jnp.concatenate(
                    [message[9 * z : 9 * z + 8, 32 * k : 32 * k + 32] for z in range(16)], 1
                )
            )
        points = jnp.concatenate(pieces, 0)
        last = jnp.concatenate([message[9 * z + 8 : 9 * z + 9, 0:32] for z in range(16)], 1)
        weight = jnp.concatenate([message[9 * z + 8 : 9 * z + 9, 32:64] for z in range(16)], 1)
        squares = jnp.sum(points * points, 0, keepdims=True)
        ones = jnp.ones_like(squares)
        zeros = jnp.zeros((6, squares.shape[1]), F32)
        features = jnp.concatenate([points, squares, ones, zeros], 0)
        log_source = jnp.log(weight) - log_sources
        features_out[...] = features
        log_out[...] = log_source
        former[...] = former_stack(
            core[...], features, log_source + last * (1.0 / EPSILON), 1.0
        )
        total[...] = jnp.zeros_like(total)
        width = columns.shape[1] // blocks

        def step(b, _):
            at = pl.multiple_of(b * width, width)
            stack = columns[:, pl.ds(at, width)]
            plan = jnp.exp2(dot(former[...], stack, ((0,), (0,))))
            high = plan.astype(BF16)
            low = (plan - high.astype(F32)).astype(BF16)
            total[...] += dot(high, stack, ((1,), (1,))) + dot(low, stack, ((1,), (1,)))
            return 0

        lax.fori_loop(0, blocks, step, 0)
        carried = (
            total[:, 0:PAD] + total[:, 2 * PAD : 3 * PAD] + total[:, 4 * PAD : 5 * PAD]
        )
        right = jnp.concatenate([points, ones, squares, zeros], 0)
        core_part = dot(right, carried, ((1,), (0,)), HIGHEST)
        col = lax.broadcasted_iota(jnp.int32, core_part.shape, 1)
        ahead = jnp.concatenate([core_part[:, 1:], core_part[:, :1]], 1)
        behind = jnp.concatenate([core_part[:, -1:], core_part[:, :-1]], 1)
        core_part = jnp.where(col == 32, ahead, jnp.where(col == 33, behind, core_part))
        core_part = jnp.where(col < 34, core_part, 0.0)
        both = jnp.concatenate(
            [core_part[12 * g : 12 * g + 12] for g in range(3)] + [jnp.zeros((12, 8), F32)], 1
        )
        for k in range(packed.shape[0] // 12):
            packed[12 * k : 12 * k + 12, :] = both

    return body


def row_kernel(blocks):
    def body(parts, features, columns, out, core_out, former, scores):
        both = parts[0:12, :]
        for k in range(1, parts.shape[0] // 12):
            both = both + parts[12 * k : 12 * k + 12, :]
        core = jnp.concatenate([both[:, PAD * g : PAD * g + PAD] for g in range(3)], 0)
        core = jnp.concatenate([core, jnp.zeros((PAD - 36, PAD), F32)], 0)
        core_out[...] = core
        former[...] = former_stack(core, features[...], None, 1.0)
        width = columns.shape[1] // blocks
        rows = features.shape[1]

        def fill(b, highest):
            at = pl.multiple_of(b * width, width)
            tile = dot(former[...], columns[:, pl.ds(at, width)], ((0,), (0,)))
            scores[:, pl.ds(at, width)] = tile
            for k in range(width // LANES):
                highest = jnp.maximum(highest, tile[:, LANES * k : LANES * k + LANES])
            return highest

        highest = lax.fori_loop(0, blocks, fill, jnp.full((rows, LANES), -jnp.inf, F32))
        highest = jnp.max(highest, 1, keepdims=True)

        def add(b, total):
            at = pl.multiple_of(b * width, width)
            tile = jnp.exp2(scores[:, pl.ds(at, width)] - highest)
            for k in range(width // LANES):
                total = total + tile[:, LANES * k : LANES * k + LANES]
            return total

        total = lax.fori_loop(0, blocks, add, jnp.zeros((rows, LANES), F32))
        total = jnp.sum(total, 1, keepdims=True)
        part = highest * LN2 + jnp.log(total)
        wide = jnp.broadcast_to(part, (rows, LANES))
        flat = [jnp.transpose(wide[LANES * k : LANES * k + LANES])[0:1] for k in range(4)]
        both = jnp.concatenate(flat, 0)
        for k in range(out.shape[0] // 4):
            out[4 * k : 4 * k + 4, :] = both

    return body


def combined(values):
    highest = functools_max(values)
    total = sum(jnp.exp(v - highest) for v in values)
    return highest + jnp.log(total)


def functools_max(values):
    highest = values[0]
    for v in values[1:]:
        highest = jnp.maximum(highest, v)
    return highest


def column_kernel(blocks):
    def body(where, parts, features, log_source, core, columns, source_out, out, former, held):
        merged = combined([parts[4 * k : 4 * k + 4, :] for k in range(parts.shape[0] // 4)])
        merged = jnp.concatenate([merged[k : k + 1] for k in range(4)], 1)
        logs = log_source[...]
        source_new = EPSILON * (logs - merged)
        source_out[...] = source_new
        former[...] = former_stack(
            core[...], features[...], logs + source_new * (1.0 / EPSILON), 0.0
        )
        width = columns.shape[1] // blocks
        per_piece = 1024 // width

        for b in range(blocks):
            tile = dot(former[...], columns[:, width * b : width * b + width], ((0,), (0,)))
            highest = jnp.max(tile, 0, keepdims=True)
            total = jnp.sum(jnp.exp2(tile - highest), 0, keepdims=True)
            part = highest * LN2 + jnp.log(total)
            for k in range(width // LANES):
                at = (b * width + LANES * k) // LANES
                held[at : at + 1, :] = part[:, LANES * k : LANES * k + LANES]
        for y in range(4):
            piece = held[8 * y : 8 * y + 8, :]
            for s in range(8):
                at = 8 * (4 * s + y)
                out[at : at + 8, :] = piece

    return body


def last_kernel(log_targets):
    def body(parts, weight, out):
        merged = combined([parts[8 * k : 8 * k + 8, :] for k in range(parts.shape[0] // 8)])
        out[...] = EPSILON * (jnp.log(weight[...]) - log_targets - merged)

    return body


def turned(core):
    core = jnp.concatenate([core[2:], core[:2]], 0)
    return jnp.concatenate([core[:, 2:], core[:, :2]], 1)


def turned_back(core):
    core = jnp.concatenate([core[32:34], core[:32]], 0)
    return jnp.concatenate([core[:, 32:34], core[:, :32]], 1)


def on_device(
    source_points,
    target_points,
    source_potential,
    target_potential,
    source_weight,
    target_weight,
    core_previous,
):
    emb, own = source_points.shape
    dims, span = target_points.shape
    n_z, n_y, n_src = lax.axis_size("z"), lax.axis_size("y"), lax.axis_size(("x", "core"))
    n_plane = n_src * n_y
    rows, columns = own * n_z, span * n_y
    log_sources = math.log(own * n_z * n_plane)
    log_targets = math.log(span * n_z * n_y)
    where = jnp.stack([lax.axis_index(("x", "core")), lax.axis_index("y")]).astype(jnp.int32)
    z = lax.axis_index("z")

    (mine,) = call(
        pack_rows,
        [((9 * n_z, LANES), F32)],
        0,
        (source_points, source_potential.reshape(1, own), source_weight.reshape(1, own)),
        name="pack_rows",
    )
    (theirs,) = call(
        pack_columns,
        [((34 * n_plane, LANES), F32)],
        1,
        (where, target_points, target_potential.reshape(8, LANES), target_weight.reshape(8, LANES)),
        scratch=[pltpu.VMEM((40, LANES), F32)],
        name="pack_columns",
    )
    theirs = exchange(theirs.reshape(n_plane, 1, 34 * LANES), PLANE).reshape(-1, LANES)
    mine = exchange(mine.reshape(n_z, 1, 9 * LANES), "z").reshape(-1, LANES)
    (stack,) = call(
        column_stack(log_targets), [((DEPTH, columns), BF16)], 0, (theirs,), name="column_stack"
    )
    previous = jnp.pad(turned(core_previous), ((0, PAD - 34), (0, PAD - 34)))
    former = pltpu.VMEM((DEPTH, rows), BF16)
    packed, features, log_source = call(
        core_kernel(log_sources, 8),
        [((12 * n_plane, LANES), F32), ((PAD, rows), F32), ((1, rows), F32)],
        0,
        (mine, stack, previous),
        scratch=[former, pltpu.VMEM((rows, DEPTH), F32)],
        name="core",
    )
    parts = exchange(packed.reshape(n_plane, 1, 12 * LANES), PLANE)
    parts = jnp.broadcast_to(jnp.sum(parts, 0, keepdims=True), (n_z, 1, 12 * LANES))
    parts = exchange(parts, "z").reshape(-1, LANES)

    row_parts, core_new = call(
        row_kernel(8),
        [((4 * n_z, LANES), F32), ((PAD, PAD), F32)],
        0,
        (parts, features, stack),
        scratch=[former, pltpu.VMEM((rows, columns), F32)],
        name="rows",
    )
    row_parts = exchange(row_parts.reshape(n_z, 1, rows), "z").reshape(-1, LANES)
    source_new, column_parts = call(
        column_kernel(8),
        [((1, rows), F32), ((8 * n_plane, LANES), F32)],
        1,
        (where, row_parts, features, log_source, core_new, stack),
        scratch=[former, pltpu.VMEM((columns // LANES, LANES), F32)],
        name="columns",
    )
    column_parts = exchange(column_parts.reshape(n_plane, 1, span), PLANE).reshape(-1, LANES)
    (target_new,) = call(
        last_kernel(log_targets),
        [((8, LANES), F32)],
        0,
        (column_parts, target_weight.reshape(8, LANES)),
        name="last",
    )
    own_rows = lax.dynamic_slice_in_dim(source_new.reshape(rows), z * own, own)
    return (own_rows, target_new.reshape(span), turned_back(core_new))


def solution(mesh):
    finer = Mesh(mesh.devices.reshape(4, 2, 4, 16), ALL)
    source, target = P(ALL), P(("y", "z"))
    placed = (
        P(None, ALL),
        P(("x", "core"), ("y", "z")),
        source,
        target,
        source,
        target,
        P(),
    )
    return jax.shard_map(
        on_device, mesh=finer, in_specs=placed, out_specs=(source, target, P()), check_vma=False
    )
```

```python
import math

import jax
import jax.numpy as jnp
from jax import lax
from jax.experimental import pallas as pl
from jax.experimental.pallas import tpu as pltpu
from jax.sharding import Mesh
from jax.sharding import PartitionSpec as P

PLANE = ("x", "core", "y")
ALL = ("x", "core", "y", "z")
EPSILON = 0.5
HIGHEST = lax.Precision.HIGHEST
LANES = 128
PAD = 40
DEPTH = 256
LOG2E = math.log2(math.e)
LN2 = math.log(2.0)
F32, BF16 = jnp.float32, jnp.bfloat16
VMEM = pl.BlockSpec(memory_space=pltpu.VMEM)
SMEM = pl.BlockSpec(memory_space=pltpu.SMEM)


def call(body, outs, n_smem, args, scratch=()):
    specs = [SMEM] * n_smem + [VMEM] * (len(args) - n_smem)
    return pl.pallas_call(
        body,
        out_shape=tuple(jax.ShapeDtypeStruct(s, d) for s, d in outs),
        in_specs=specs,
        out_specs=tuple(VMEM for _ in outs),
        scratch_shapes=list(scratch),
        compiler_params=pltpu.CompilerParams(vmem_limit_bytes=48 * 2**20),
    )(*args)


def exchange(copies, axis):
    return lax.all_to_all(copies, axis, split_axis=0, concat_axis=0, tiled=True)


def dot(former, latter, dims, precision=None):
    return lax.dot_general(
        former, latter, (dims, ((), ())), precision=precision, preferred_element_type=F32
    )


def split(value):
    first = value.astype(BF16).astype(F32)
    rest = value - first
    second = rest.astype(BF16).astype(F32)
    return first, second, rest - second


def stacked(pieces, order):
    blocks = [pieces[k] for k in order]
    filler = jnp.zeros((DEPTH - PAD * len(order), pieces[0].shape[1]), F32)
    return jnp.concatenate([*blocks, filler], 0).astype(BF16)


LATTER_ORDER = (0, 0, 1, 0, 2, 1)
FORMER_ORDER = (0, 1, 0, 2, 0, 1)


def pack(where, *refs):
    given, (out, column_out), held, (sem, *into) = refs[:6], refs[6:8], refs[8], refs[9:]
    copies = [pltpu.make_async_copy(a, b, sem.at[k]) for k, (a, b) in enumerate(zip(given, into))]
    for copy in copies:
        copy.start()
    for copy in copies:
        copy.wait()
    points, potential, weight, column_points, column_potential, column_weight = into
    value = points[...]
    block = jnp.concatenate([value[8 * k : 8 * k + 8] for k in range(4)], axis=1)
    last = jnp.concatenate(
        [potential[...], weight[...], jnp.ones((1, LANES - 64), F32)], axis=1
    )
    both = jnp.concatenate([block, last], 0)
    for k in range(out.shape[0] // 9):
        out[9 * k : 9 * k + 9, :] = both
    for r in range(4):
        for k in range(8):
            held[8 * r + k : 8 * r + k + 1, :] = column_points[
                r : r + 1, LANES * k : LANES * k + LANES
            ]
    src = where[0]
    held[32:33, :] = column_potential[pl.ds(src, 1), :]
    held[33:34, :] = column_weight[pl.ds(src, 1), :]
    both = held[0:34, :]
    for k in range(column_out.shape[0] // 34):
        column_out[34 * k : 34 * k + 34, :] = both


def column_stack(log_targets):
    def body(*refs):
        *messages, out = refs
        for y, message in enumerate(messages):
            for k in range(8):
                points = jnp.concatenate(
                    [message[pl.ds(34 * s + k, 4, stride=8), :] for s in range(8)], 0
                )
                squares = jnp.sum(points * points, 0, keepdims=True)
                at = 34 * k + 32
                offset = jnp.log(message[at + 1 : at + 2, :]) - log_targets
                offset = (offset + message[at : at + 1, :] * (1.0 / EPSILON)) * LOG2E
                tail = jnp.concatenate(
                    [squares, jnp.ones((1, LANES), F32), offset, jnp.zeros((5, LANES), F32)], 0
                )
                value = jnp.concatenate([points, tail], 0)
                col = 1024 * y + LANES * k
                out[:, col : col + LANES] = stacked(split(value), LATTER_ORDER)

    return body


def signs(core):
    row = lax.broadcasted_iota(jnp.int32, core.shape, 0)
    col = lax.broadcasted_iota(jnp.int32, core.shape, 1)
    core = jnp.where(row < 32, -2.0 * core, core)
    return jnp.where(col < 32, -2.0 * core, core)


def former_stack(core, features, row_term, column_factor):
    weighted = dot(signs(core), features, ((0,), (0,)), HIGHEST) * (2.0 / EPSILON * LOG2E)
    row = lax.broadcasted_iota(jnp.int32, weighted.shape, 0)
    if row_term is not None:
        weighted = jnp.where(row == 33, weighted + row_term * LOG2E, weighted)
    weighted = jnp.where(row == 34, column_factor, weighted)
    return stacked(split(weighted), FORMER_ORDER)


def core_kernel(log_sources, blocks):
    def body(message, columns, core, packed, features_out, log_out, former, total):
        pieces = []
        for k in range(4):
            pieces.append(
                jnp.concatenate(
                    [message[9 * z : 9 * z + 8, 32 * k : 32 * k + 32] for z in range(16)], 1
                )
            )
        points = jnp.concatenate(pieces, 0)
        last = jnp.concatenate([message[9 * z + 8 : 9 * z + 9, 0:32] for z in range(16)], 1)
        weight = jnp.concatenate([message[9 * z + 8 : 9 * z + 9, 32:64] for z in range(16)], 1)
        squares = jnp.sum(points * points, 0, keepdims=True)
        ones = jnp.ones_like(squares)
        zeros = jnp.zeros((6, squares.shape[1]), F32)
        features = jnp.concatenate([points, squares, ones, zeros], 0)
        log_source = jnp.log(weight) - log_sources
        features_out[...] = features
        log_out[...] = log_source
        former[...] = former_stack(
            core[...], features, log_source + last * (1.0 / EPSILON), 1.0
        )
        total[...] = jnp.zeros_like(total)
        width = columns.shape[1] // blocks

        def step(b, _):
            at = pl.multiple_of(b * width, width)
            stack = columns[:, pl.ds(at, width)]
            plan = jnp.exp2(dot(former[...], stack, ((0,), (0,))))
            high = plan.astype(BF16)
            low = (plan - high.astype(F32)).astype(BF16)
            total[...] += dot(high, stack, ((1,), (1,))) + dot(low, stack, ((1,), (1,)))
            return 0

        lax.fori_loop(0, blocks, step, 0)
        carried = (
            total[:, 0:PAD] + total[:, 2 * PAD : 3 * PAD] + total[:, 4 * PAD : 5 * PAD]
        )
        right = jnp.concatenate([points, ones, squares, zeros], 0)
        core_part = dot(right, carried, ((1,), (0,)), HIGHEST)
        col = lax.broadcasted_iota(jnp.int32, core_part.shape, 1)
        ahead = jnp.concatenate([core_part[:, 1:], core_part[:, :1]], 1)
        behind = jnp.concatenate([core_part[:, -1:], core_part[:, :-1]], 1)
        core_part = jnp.where(col == 32, ahead, jnp.where(col == 33, behind, core_part))
        core_part = jnp.where(col < 34, core_part, 0.0)
        both = jnp.concatenate(
            [core_part[12 * g : 12 * g + 12] for g in range(3)] + [jnp.zeros((12, 8), F32)], 1
        )
        for k in range(packed.shape[0] // 12):
            packed[12 * k : 12 * k + 12, :] = both

    return body


def row_kernel(blocks):
    def body(parts, features, columns, out, core_out, former, scores):
        both = parts[0:12, :]
        for k in range(1, parts.shape[0] // 12):
            both = both + parts[12 * k : 12 * k + 12, :]
        core = jnp.concatenate([both[:, PAD * g : PAD * g + PAD] for g in range(3)], 0)
        core = jnp.concatenate([core, jnp.zeros((PAD - 36, PAD), F32)], 0)
        core_out[...] = core
        former[...] = former_stack(core, features[...], None, 1.0)
        width = columns.shape[1] // blocks
        rows = features.shape[1]

        def fill(b, highest):
            at = pl.multiple_of(b * width, width)
            tile = dot(former[...], columns[:, pl.ds(at, width)], ((0,), (0,)))
            scores[:, pl.ds(at, width)] = tile
            for k in range(width // LANES):
                highest = jnp.maximum(highest, tile[:, LANES * k : LANES * k + LANES])
            return highest

        highest = lax.fori_loop(0, blocks, fill, jnp.full((rows, LANES), -jnp.inf, F32))
        highest = jnp.max(highest, 1, keepdims=True)

        def add(b, total):
            at = pl.multiple_of(b * width, width)
            tile = jnp.exp2(scores[:, pl.ds(at, width)] - highest)
            for k in range(width // LANES):
                total = total + tile[:, LANES * k : LANES * k + LANES]
            return total

        total = lax.fori_loop(0, blocks, add, jnp.zeros((rows, LANES), F32))
        total = jnp.sum(total, 1, keepdims=True)
        part = highest * LN2 + jnp.log(total)
        wide = jnp.broadcast_to(part, (rows, LANES))
        flat = [jnp.transpose(wide[LANES * k : LANES * k + LANES])[0:1] for k in range(4)]
        both = jnp.concatenate(flat, 0)
        for k in range(out.shape[0] // 4):
            out[4 * k : 4 * k + 4, :] = both

    return body


def combined(values):
    highest = functools_max(values)
    total = sum(jnp.exp(v - highest) for v in values)
    return highest + jnp.log(total)


def functools_max(values):
    highest = values[0]
    for v in values[1:]:
        highest = jnp.maximum(highest, v)
    return highest


def column_kernel(blocks):
    def body(where, parts, features, log_source, core, columns, source_out, out, former, held):
        merged = combined([parts[4 * k : 4 * k + 4, :] for k in range(parts.shape[0] // 4)])
        merged = jnp.concatenate([merged[k : k + 1] for k in range(4)], 1)
        logs = log_source[...]
        source_new = EPSILON * (logs - merged)
        source_out[...] = source_new
        former[...] = former_stack(
            core[...], features[...], logs + source_new * (1.0 / EPSILON), 0.0
        )
        width = columns.shape[1] // blocks

        for b in range(blocks):
            tile = dot(former[...], columns[:, width * b : width * b + width], ((0,), (0,)))
            highest = jnp.max(tile, 0, keepdims=True)
            total = jnp.sum(jnp.exp2(tile - highest), 0, keepdims=True)
            part = highest * LN2 + jnp.log(total)
            for k in range(width // LANES):
                at = (b * width + LANES * k) // LANES
                held[at : at + 1, :] = part[:, LANES * k : LANES * k + LANES]
        for y in range(4):
            turn = lax.rem(where[1] - y + 4, 4)
            piece = held[pl.ds(pl.multiple_of(8 * turn, 8), 8), :]
            for s in range(8):
                at = 8 * (4 * s + y)
                out[at : at + 8, :] = piece

    return body


def last_kernel(log_targets):
    def body(parts, weight, out):
        merged = combined([parts[8 * k : 8 * k + 8, :] for k in range(parts.shape[0] // 8)])
        out[...] = EPSILON * (jnp.log(weight[...]) - log_targets - merged)

    return body


def turned(core):
    core = jnp.concatenate([core[2:], core[:2]], 0)
    return jnp.concatenate([core[:, 2:], core[:, :2]], 1)


def turned_back(core):
    core = jnp.concatenate([core[32:34], core[:32]], 0)
    return jnp.concatenate([core[:, 32:34], core[:, :32]], 1)


def on_device(
    source_points,
    target_points,
    source_potential,
    target_potential,
    source_weight,
    target_weight,
    core_previous,
):
    _, own = source_points.shape
    _, span = target_points.shape
    n_z, n_y, n_src = lax.axis_size("z"), lax.axis_size("y"), lax.axis_size(("x", "core"))
    n_plane = n_src * n_y
    rows, columns = own * n_z, span * n_y
    log_sources = math.log(own * n_z * n_plane)
    log_targets = math.log(span * n_z * n_y)
    where = jnp.stack([lax.axis_index(("x", "core")), lax.axis_index("y")]).astype(jnp.int32)
    z = lax.axis_index("z")

    given = (
        source_points,
        source_potential.reshape(1, own),
        source_weight.reshape(1, own),
        target_points,
        target_potential.reshape(8, LANES),
        target_weight.reshape(8, LANES),
    )
    mine, theirs = pl.pallas_call(
        pack,
        out_shape=(
            jax.ShapeDtypeStruct((9 * n_z, LANES), F32),
            jax.ShapeDtypeStruct((34 * n_src, LANES), F32),
        ),
        in_specs=[SMEM] + [pl.BlockSpec(memory_space=pl.ANY)] * len(given),
        out_specs=(VMEM, VMEM),
        scratch_shapes=[
            pltpu.VMEM((PAD, LANES), F32),
            pltpu.SemaphoreType.DMA((len(given),)),
            *(pltpu.VMEM(a.shape, F32) for a in given),
        ],
        name="pack",
    )(where, *given)
    theirs = exchange(theirs.reshape(n_src, 1, 34 * LANES), ("x", "core"))
    mine = exchange(mine.reshape(n_z, 1, 9 * LANES), "z").reshape(-1, LANES)
    turns = [
        lax.ppermute(theirs, "y", [(i, (i + k) % n_y) for i in range(n_y)])
        for k in range(1, n_y)
    ]
    messages = [m.reshape(-1, LANES) for m in (theirs, *turns)]
    (stack,) = call(column_stack(log_targets), [((DEPTH, columns), BF16)], 0, messages)
    previous = jnp.pad(turned(core_previous), ((0, PAD - 34), (0, PAD - 34)))
    former = pltpu.VMEM((DEPTH, rows), BF16)
    packed, features, log_source = call(
        core_kernel(log_sources, 8),
        [((12 * n_plane, LANES), F32), ((PAD, rows), F32), ((1, rows), F32)],
        0,
        (mine, stack, previous),
        scratch=[former, pltpu.VMEM((rows, DEPTH), F32)],
    )
    parts = exchange(packed.reshape(n_plane, 1, 12 * LANES), PLANE)
    parts = jnp.broadcast_to(jnp.sum(parts, 0, keepdims=True), (n_z, 1, 12 * LANES))
    parts = exchange(parts, "z").reshape(-1, LANES)

    row_parts, core_new = call(
        row_kernel(8),
        [((4 * n_z, LANES), F32), ((PAD, PAD), F32)],
        0,
        (parts, features, stack),
        scratch=[former, pltpu.VMEM((rows, columns), F32)],
    )
    row_parts = exchange(row_parts.reshape(n_z, 1, rows), "z").reshape(-1, LANES)
    source_new, column_parts = call(
        column_kernel(8),
        [((1, rows), F32), ((8 * n_plane, LANES), F32)],
        1,
        (where, row_parts, features, log_source, core_new, stack),
        scratch=[former, pltpu.VMEM((columns // LANES, LANES), F32)],
    )
    column_parts = exchange(column_parts.reshape(n_plane, 1, span), PLANE).reshape(-1, LANES)
    (target_new,) = call(
        last_kernel(log_targets),
        [((8, LANES), F32)],
        0,
        (column_parts, target_weight.reshape(8, LANES)),
    )
    own_rows = lax.dynamic_slice_in_dim(source_new.reshape(rows), z * own, own)
    return (own_rows, target_new.reshape(span), turned_back(core_new))


def solution(mesh):
    finer = Mesh(mesh.devices.reshape(4, 2, 4, 16), ALL)
    source, target = P(ALL), P(("y", "z"))
    placed = (
        P(None, ALL),
        P(("x", "core"), ("y", "z")),
        source,
        target,
        source,
        target,
        P(),
    )
    return jax.shard_map(
        on_device, mesh=finer, in_specs=placed, out_specs=(source, target, P()), check_vma=False
    )
```

```python
import functools
import math

import jax
import jax.numpy as jnp
from jax import lax
from jax.experimental import pallas as pl
from jax.experimental.pallas import tpu as pltpu
from jax.sharding import Mesh
from jax.sharding import PartitionSpec as P

PLANE = ("x", "core", "y")
ALL = ("x", "core", "y", "z")
EPSILON = 0.5
HIGHEST = lax.Precision.HIGHEST
LANES = 128
PAD = 40
DEPTH = 256
LOG2E = math.log2(math.e)
LN2 = math.log(2.0)
F32, BF16 = jnp.float32, jnp.bfloat16
VMEM = pl.BlockSpec(memory_space=pltpu.VMEM)


def call(body, outs, args, scratch=(), name=None):
    return pl.pallas_call(
        body,
        out_shape=tuple(jax.ShapeDtypeStruct(s, d) for s, d in outs),
        in_specs=[VMEM] * len(args),
        out_specs=tuple(VMEM for _ in outs),
        scratch_shapes=list(scratch),
        compiler_params=pltpu.CompilerParams(vmem_limit_bytes=48 * 2**20),
        name=name,
    )(*args)


def exchange(copies, axis):
    return lax.all_to_all(copies, axis, split_axis=0, concat_axis=0, tiled=True)


def dot(former, latter, dims, precision=None):
    return lax.dot_general(
        former, latter, (dims, ((), ())), precision=precision, preferred_element_type=F32
    )


def split(value):
    first = value.astype(BF16).astype(F32)
    rest = value - first
    second = rest.astype(BF16).astype(F32)
    return first, second, rest - second


def stacked(pieces, order):
    blocks = [pieces[k] for k in order]
    filler = jnp.zeros((DEPTH - PAD * len(order), pieces[0].shape[1]), F32)
    return jnp.concatenate([*blocks, filler], 0).astype(BF16)


LATTER_ORDER = (0, 0, 1, 0, 2, 1)
FORMER_ORDER = (0, 1, 0, 2, 0, 1)


def pack(*refs):
    given, (out, column_out), held, (sem, *into) = refs[:6], refs[6:8], refs[8], refs[9:]
    copies = [pltpu.make_async_copy(a, b, sem.at[k]) for k, (a, b) in enumerate(zip(given, into))]
    for copy in copies:
        copy.start()
    for copy in copies:
        copy.wait()
    points, potential, weight, column_points, column_potential, column_weight = into
    value = points[...]
    block = jnp.concatenate([value[8 * k : 8 * k + 8] for k in range(4)], axis=1)
    last = jnp.concatenate(
        [potential[...], weight[...], jnp.ones((1, LANES - 64), F32)], axis=1
    )
    both = jnp.concatenate([block, last], 0)
    for k in range(out.shape[0] // 9):
        out[9 * k : 9 * k + 9, :] = both
    for r in range(4):
        for k in range(8):
            held[8 * r + k : 8 * r + k + 1, :] = column_points[
                r : r + 1, LANES * k : LANES * k + LANES
            ]
    src = lax.axis_index(("x", "core"))
    held[32:33, :] = column_potential[pl.ds(src, 1), :]
    held[33:34, :] = column_weight[pl.ds(src, 1), :]
    both = held[0:34, :]
    for k in range(column_out.shape[0] // 34):
        column_out[34 * k : 34 * k + 34, :] = both


def column_stack(message, out, log_targets):
    def step(y, _):
        for k in range(8):
            points = jnp.concatenate(
                [message[pl.ds(34 * (4 * s + y) + k, 4, stride=8), :] for s in range(8)], 0
            )
            squares = jnp.sum(points * points, 0, keepdims=True)
            at = 34 * (4 * k + y) + 32
            offset = jnp.log(message[pl.ds(at + 1, 1), :]) - log_targets
            offset = (offset + message[pl.ds(at, 1), :] * (1.0 / EPSILON)) * LOG2E
            tail = jnp.concatenate(
                [squares, jnp.ones((1, LANES), F32), offset, jnp.zeros((5, LANES), F32)], 0
            )
            value = jnp.concatenate([points, tail], 0)
            col = pl.multiple_of(1024 * y + LANES * k, LANES)
            out[:, pl.ds(col, LANES)] = stacked(split(value), LATTER_ORDER)
        return 0

    lax.fori_loop(0, 4, step, 0)


def in_turns(former, columns, consume, tiles):
    even, odd = tiles
    width = even.shape[1]
    blocks = columns.shape[1] // width

    def tile(b):
        at = pl.multiple_of(b * width, width)
        return dot(former[...], columns[:, pl.ds(at, width)], ((0,), (0,)))

    even[...] = tile(0)

    def step(i, _):
        odd[...] = tile(2 * i + 1)
        consume(even, 2 * i)
        even[...] = tile(jnp.minimum(2 * i + 2, blocks - 1))
        consume(odd, 2 * i + 1)
        return 0

    lax.fori_loop(0, blocks // 2, step, 0)


def signs(core):
    row = lax.broadcasted_iota(jnp.int32, core.shape, 0)
    col = lax.broadcasted_iota(jnp.int32, core.shape, 1)
    core = jnp.where(row < 32, -2.0 * core, core)
    return jnp.where(col < 32, -2.0 * core, core)


def former_stack(core, features, row_term, column_factor):
    weighted = dot(signs(core), features, ((0,), (0,)), HIGHEST) * (2.0 / EPSILON * LOG2E)
    row = lax.broadcasted_iota(jnp.int32, weighted.shape, 0)
    if row_term is not None:
        weighted = jnp.where(row == 33, weighted + row_term * LOG2E, weighted)
    weighted = jnp.where(row == 34, column_factor, weighted)
    return stacked(split(weighted), FORMER_ORDER)


def turned(core):
    core = jnp.concatenate([core[2:34], core[0:2], jnp.zeros((PAD - 34, 34), F32)], 0)
    return jnp.concatenate([core[:, 2:34], core[:, 0:2], jnp.zeros((PAD, PAD - 34), F32)], 1)


def turned_back(core):
    core = jnp.concatenate([core[32:34], core[0:32]], 0)
    return jnp.concatenate([core[:, 32:34], core[:, 0:32]], 1)


def core_kernel(log_sources, log_targets):
    def body(message, arrived, core, packed, features_out, log_out, columns, former, total, *tiles):
        column_stack(arrived, columns, log_targets)
        pieces = []
        for k in range(4):
            pieces.append(
                jnp.concatenate(
                    [message[9 * z : 9 * z + 8, 32 * k : 32 * k + 32] for z in range(16)], 1
                )
            )
        points = jnp.concatenate(pieces, 0)
        last = jnp.concatenate([message[9 * z + 8 : 9 * z + 9, 0:32] for z in range(16)], 1)
        weight = jnp.concatenate([message[9 * z + 8 : 9 * z + 9, 32:64] for z in range(16)], 1)
        squares = jnp.sum(points * points, 0, keepdims=True)
        ones = jnp.ones_like(squares)
        zeros = jnp.zeros((6, squares.shape[1]), F32)
        features = jnp.concatenate([points, squares, ones, zeros], 0)
        log_source = jnp.log(weight) - log_sources
        features_out[...] = features
        log_out[...] = log_source
        former[...] = former_stack(
            turned(core[...]), features, log_source + last * (1.0 / EPSILON), 1.0
        )
        total[...] = jnp.zeros_like(total)

        def consume(tile, b):
            width = tile.shape[1]
            stack = columns[:, pl.ds(pl.multiple_of(b * width, width), width)]
            plan = jnp.exp2(tile[...])
            high = plan.astype(BF16)
            low = (plan - high.astype(F32)).astype(BF16)
            total[...] += dot(high, stack, ((1,), (1,))) + dot(low, stack, ((1,), (1,)))

        in_turns(former, columns, consume, tiles)
        carried = (
            total[:, 0:PAD] + total[:, 2 * PAD : 3 * PAD] + total[:, 4 * PAD : 5 * PAD]
        )
        right = jnp.concatenate([points, ones, squares, zeros], 0)
        core_part = dot(right, carried, ((1,), (0,)), HIGHEST)
        col = lax.broadcasted_iota(jnp.int32, core_part.shape, 1)
        ahead = jnp.concatenate([core_part[:, 1:], core_part[:, :1]], 1)
        behind = jnp.concatenate([core_part[:, -1:], core_part[:, :-1]], 1)
        core_part = jnp.where(col == 32, ahead, jnp.where(col == 33, behind, core_part))
        core_part = jnp.where(col < 34, core_part, 0.0)
        both = jnp.concatenate(
            [core_part[12 * g : 12 * g + 12] for g in range(3)] + [jnp.zeros((12, 8), F32)], 1
        )
        for k in range(packed.shape[0] // 12):
            packed[12 * k : 12 * k + 12, :] = both

    return body


def row_kernel(parts, features, columns, out, core_out, core_new, former, highest, total, *tiles):
    both = parts[0:12, :]
    for k in range(1, parts.shape[0] // 12):
        both = both + parts[12 * k : 12 * k + 12, :]
    core = jnp.concatenate([both[:, PAD * g : PAD * g + PAD] for g in range(3)], 0)
    core = jnp.concatenate([core, jnp.zeros((PAD - 36, PAD), F32)], 0)
    core_out[...] = core
    core_new[...] = turned_back(core)
    former[...] = former_stack(core, features[...], None, 1.0)
    rows = features.shape[1]
    highest[...] = jnp.full(highest.shape, jnp.finfo(F32).min, F32)
    total[...] = jnp.zeros_like(total)

    def consume(tile, _):
        for r in range(0, rows, 64):
            at = pl.ds(r, 64)
            pieces = [tile[at, LANES * k : LANES * k + LANES] for k in range(tile.shape[1] // LANES)]
            before = highest[at, :]
            now = largest([before, *pieces])
            highest[at, :] = now
            total[at, :] = total[at, :] * jnp.exp2(before - now) + sum(
                jnp.exp2(p - now) for p in pieces
            )

    in_turns(former, columns, consume, tiles)
    lanes = highest[...]
    top = jnp.max(lanes, 1, keepdims=True)
    added = jnp.sum(total[...] * jnp.exp2(lanes - top), 1, keepdims=True)
    part = top * LN2 + jnp.log(added)
    wide = jnp.broadcast_to(part, (rows, LANES))
    flat = [jnp.transpose(wide[LANES * k : LANES * k + LANES])[0:1] for k in range(4)]
    both = jnp.concatenate(flat, 0)
    for k in range(out.shape[0] // 4):
        out[4 * k : 4 * k + 4, :] = both


def largest(values):
    return functools.reduce(jnp.maximum, values)


def combined(values):
    highest = largest(values)
    total = sum(jnp.exp(v - highest) for v in values)
    return highest + jnp.log(total)


def column_kernel(
    parts, features, log_source, core, columns, own_out, out, former, held, mine, *tiles
):
    merged = combined([parts[4 * k : 4 * k + 4, :] for k in range(parts.shape[0] // 4)])
    merged = jnp.concatenate([merged[k : k + 1] for k in range(4)], 1)
    logs = log_source[...]
    source_new = EPSILON * (logs - merged)
    own = own_out.shape[1]
    for k in range(mine.shape[0]):
        mine[k : k + 1, :] = source_new[:, own * k : own * k + own]
    own_out[...] = mine[pl.ds(lax.axis_index("z"), 1), :]
    former[...] = former_stack(core[...], features[...], logs + source_new * (1.0 / EPSILON), 0.0)

    def consume(tile, b):
        count = tile.shape[1] // LANES
        for k in range(count):
            piece = tile[:, LANES * k : LANES * k + LANES]
            highest = jnp.max(piece, 0, keepdims=True)
            total = jnp.sum(jnp.exp2(piece - highest), 0, keepdims=True)
            held[pl.ds(b * count + k, 1), :] = highest * LN2 + jnp.log(total)

    in_turns(former, columns, consume, tiles)
    for y in range(4):
        piece = held[8 * y : 8 * y + 8, :]
        for s in range(8):
            at = 8 * (4 * s + y)
            out[at : at + 8, :] = piece


def last_kernel(log_targets):
    def body(parts, weight, out):
        merged = combined([parts[8 * k : 8 * k + 8, :] for k in range(parts.shape[0] // 8)])
        out[...] = EPSILON * (jnp.log(weight[...]) - log_targets - merged)

    return body


def on_device(
    source_points,
    target_points,
    source_potential,
    target_potential,
    source_weight,
    target_weight,
    core_previous,
):
    emb, own = source_points.shape
    dims, span = target_points.shape
    n_z, n_y, n_src = lax.axis_size("z"), lax.axis_size("y"), lax.axis_size(("x", "core"))
    n_plane = n_src * n_y
    rows, columns = own * n_z, span * n_y
    log_sources = math.log(own * n_z * n_plane)
    log_targets = math.log(span * n_z * n_y)
    given = (
        source_points,
        source_potential.reshape(1, own),
        source_weight.reshape(1, own),
        target_points,
        target_potential.reshape(8, LANES),
        target_weight.reshape(8, LANES),
    )
    mine, theirs = pl.pallas_call(
        pack,
        out_shape=(
            jax.ShapeDtypeStruct((9 * n_z, LANES), F32),
            jax.ShapeDtypeStruct((34 * n_plane, LANES), F32),
        ),
        in_specs=[pl.BlockSpec(memory_space=pl.ANY)] * len(given),
        out_specs=(VMEM, VMEM),
        scratch_shapes=[
            pltpu.VMEM((PAD, LANES), F32),
            pltpu.SemaphoreType.DMA((len(given),)),
            *(pltpu.VMEM(a.shape, F32) for a in given),
        ],
        name="pack",
    )(*given)
    theirs = exchange(theirs.reshape(n_plane, 1, 34 * LANES), PLANE).reshape(-1, LANES)
    mine = exchange(mine.reshape(n_z, 1, 9 * LANES), "z").reshape(-1, LANES)
    former = pltpu.VMEM((DEPTH, rows), BF16)
    tiles = (pltpu.VMEM((rows, 512), F32), pltpu.VMEM((rows, 512), F32))
    packed, features, log_source, stack = call(
        core_kernel(log_sources, log_targets),
        [
            ((12 * n_plane, LANES), F32),
            ((PAD, rows), F32),
            ((1, rows), F32),
            ((DEPTH, columns), BF16),
        ],
        (mine, theirs, core_previous),
        scratch=[former, pltpu.VMEM((rows, DEPTH), F32), *tiles],
        name="core",
    )
    parts = exchange(packed.reshape(n_plane, 1, 12 * LANES), PLANE)
    parts = jnp.broadcast_to(jnp.sum(parts, 0, keepdims=True), (n_z, 1, 12 * LANES))
    parts = exchange(parts, "z").reshape(-1, LANES)

    per_lane = pltpu.VMEM((rows, LANES), F32)
    row_parts, core, core_new = call(
        row_kernel,
        [((4 * n_z, LANES), F32), ((PAD, PAD), F32), (core_previous.shape, F32)],
        (parts, features, stack),
        scratch=[former, per_lane, per_lane, *tiles],
        name="rows",
    )
    row_parts = exchange(row_parts.reshape(n_z, 1, rows), "z").reshape(-1, LANES)
    own_rows, column_parts = call(
        column_kernel,
        [((1, own), F32), ((8 * n_plane, LANES), F32)],
        (row_parts, features, log_source, core, stack),
        scratch=[
            former,
            pltpu.VMEM((columns // LANES, LANES), F32),
            pltpu.VMEM((n_z, own), F32),
            *tiles,
        ],
        name="columns",
    )
    column_parts = exchange(column_parts.reshape(n_plane, 1, span), PLANE).reshape(-1, LANES)
    (target_new,) = call(
        last_kernel(log_targets),
        [((8, LANES), F32)],
        (column_parts, target_weight.reshape(8, LANES)),
        name="last",
    )
    return (own_rows.reshape(own), target_new.reshape(span), core_new)


def solution(mesh):
    finer = Mesh(mesh.devices.reshape(4, 2, 4, 16), ALL)
    source, target = P(ALL), P(("y", "z"))
    placed = (
        P(None, ALL),
        P(("x", "core"), ("y", "z")),
        source,
        target,
        source,
        target,
        P(),
    )
    return jax.shard_map(
        on_device, mesh=finer, in_specs=placed, out_specs=(source, target, P()), check_vma=False
    )
```

```python
import functools
import math

import jax
import jax.numpy as jnp
from jax import lax
from jax.experimental import pallas as pl
from jax.experimental.pallas import tpu as pltpu
from jax.sharding import Mesh
from jax.sharding import PartitionSpec as P

PLANE = ("x", "core", "y")
ALL = ("x", "core", "y", "z")
EPSILON = 0.5
HIGHEST = lax.Precision.HIGHEST
LANES = 128
PAD = 40
DEPTH = 256
LOG2E = math.log2(math.e)
LN2 = math.log(2.0)
FLOOR = 2.0**-60
F32, BF16 = jnp.float32, jnp.bfloat16
VMEM = pl.BlockSpec(memory_space=pltpu.VMEM)


def call(body, outs, args, scratch=(), name=None, grant=8):
    return pl.pallas_call(
        body,
        out_shape=tuple(jax.ShapeDtypeStruct(s, d) for s, d in outs),
        in_specs=[VMEM] * len(args),
        out_specs=tuple(VMEM for _ in outs),
        scratch_shapes=list(scratch),
        compiler_params=pltpu.CompilerParams(vmem_limit_bytes=grant * 2**20),
        name=name,
    )(*args)


def exchange(copies, axis):
    return lax.all_to_all(copies, axis, split_axis=0, concat_axis=0, tiled=True)


def dot(former, latter, dims, precision=None):
    return lax.dot_general(
        former, latter, (dims, ((), ())), precision=precision, preferred_element_type=F32
    )


def split(value):
    first = value.astype(BF16).astype(F32)
    rest = value - first
    second = rest.astype(BF16).astype(F32)
    return first, second, rest - second


def stacked(pieces, order):
    blocks = [pieces[k] for k in order]
    filler = jnp.zeros((DEPTH - PAD * len(order), pieces[0].shape[1]), F32)
    return jnp.concatenate([*blocks, filler], 0).astype(BF16)


LATTER_ORDER = (0, 0, 1, 0, 2, 1)
FORMER_ORDER = (0, 1, 0, 2, 0, 1)


def pack(*refs):
    given, (out, column_out, core_out), (held, sem, *into) = refs[:7], refs[7:10], refs[10:]
    copies = [pltpu.make_async_copy(a, b, sem.at[k]) for k, (a, b) in enumerate(zip(given, into))]
    for copy in copies:
        copy.start()
    for copy in copies:
        copy.wait()
    points, potential, weight, column_points, column_potential, column_weight, core = into
    core_out[...] = turned(core[...])
    value = points[...]
    block = jnp.concatenate([value[8 * k : 8 * k + 8] for k in range(4)], axis=1)
    last = jnp.concatenate(
        [potential[...], weight[...], jnp.ones((1, LANES - 64), F32)], axis=1
    )
    both = jnp.concatenate([block, last], 0)
    for k in range(out.shape[0] // 9):
        out[9 * k : 9 * k + 9, :] = both
    for r in range(4):
        for k in range(8):
            held[8 * r + k : 8 * r + k + 1, :] = column_points[
                r : r + 1, LANES * k : LANES * k + LANES
            ]
    src = lax.axis_index(("x", "core"))
    held[32:33, :] = column_potential[pl.ds(src, 1), :]
    held[33:34, :] = column_weight[pl.ds(src, 1), :]
    both = held[0:34, :]
    for k in range(column_out.shape[0] // 34):
        column_out[34 * k : 34 * k + 34, :] = both


def column_stack(message, out, log_targets):
    def step(y, _):
        for k in range(8):
            points = jnp.concatenate(
                [message[pl.ds(34 * (4 * s + y) + k, 4, stride=8), :] for s in range(8)], 0
            )
            squares = jnp.sum(points * points, 0, keepdims=True)
            at = 34 * (4 * k + y) + 32
            offset = jnp.log(message[pl.ds(at + 1, 1), :]) - log_targets
            offset = (offset + message[pl.ds(at, 1), :] * (1.0 / EPSILON)) * LOG2E
            tail = jnp.concatenate(
                [squares, jnp.ones((1, LANES), F32), offset, jnp.zeros((5, LANES), F32)], 0
            )
            value = jnp.concatenate([points, tail], 0)
            col = pl.multiple_of(1024 * y + LANES * k, LANES)
            out[:, pl.ds(col, LANES)] = stacked(split(value), LATTER_ORDER)
        return 0

    lax.fori_loop(0, 4, step, 0)


def in_turns(former, columns, consume, tiles):
    even, odd = tiles
    width = even.shape[1]
    blocks = columns.shape[1] // width

    def tile(b):
        at = pl.multiple_of(b * width, width)
        return dot(former[...], columns[:, pl.ds(at, width)], ((0,), (0,)))

    even[...] = tile(0)

    def step(i, _):
        odd[...] = tile(2 * i + 1)
        consume(even, 2 * i)
        even[...] = tile(jnp.minimum(2 * i + 2, blocks - 1))
        consume(odd, 2 * i + 1)
        return 0

    lax.fori_loop(0, blocks // 2, step, 0)


def signs(core):
    row = lax.broadcasted_iota(jnp.int32, core.shape, 0)
    col = lax.broadcasted_iota(jnp.int32, core.shape, 1)
    core = jnp.where(row < 32, -2.0 * core, core)
    return jnp.where(col < 32, -2.0 * core, core)


def weighted_core(core, features):
    return dot(signs(core), features, ((0,), (0,)), HIGHEST) * (2.0 / EPSILON * LOG2E)


def former_stack(weighted, row_term, column_factor):
    row = lax.broadcasted_iota(jnp.int32, weighted.shape, 0)
    if row_term is not None:
        weighted = jnp.where(row == 33, weighted + row_term * LOG2E, weighted)
    weighted = jnp.where(row == 34, column_factor, weighted)
    return stacked(split(weighted), FORMER_ORDER)


def turned(core):
    core = jnp.concatenate([core[2:34], core[0:2], jnp.zeros((PAD - 34, 34), F32)], 0)
    return jnp.concatenate([core[:, 2:34], core[:, 0:2], jnp.zeros((PAD, PAD - 34), F32)], 1)


def turned_back(core):
    core = jnp.concatenate([core[32:34], core[0:32]], 0)
    return jnp.concatenate([core[:, 32:34], core[:, 0:32]], 1)


def source_kernel(log_sources):
    def body(message, core, features_out, log_out, former):
        pieces = []
        for k in range(4):
            pieces.append(
                jnp.concatenate(
                    [message[9 * z : 9 * z + 8, 32 * k : 32 * k + 32] for z in range(16)], 1
                )
            )
        points = jnp.concatenate(pieces, 0)
        last = jnp.concatenate([message[9 * z + 8 : 9 * z + 9, 0:32] for z in range(16)], 1)
        weight = jnp.concatenate([message[9 * z + 8 : 9 * z + 9, 32:64] for z in range(16)], 1)
        squares = jnp.sum(points * points, 0, keepdims=True)
        ones = jnp.ones_like(squares)
        zeros = jnp.zeros((6, squares.shape[1]), F32)
        features = jnp.concatenate([points, squares, ones, zeros], 0)
        log_source = jnp.log(weight) - log_sources
        features_out[...] = features
        log_out[...] = log_source
        former[...] = former_stack(
            weighted_core(core[...], features), log_source + last * (1.0 / EPSILON), 1.0
        )

    return body


def core_to_rows(core):
    tail = jnp.concatenate(
        [core[30:34, 0:26], jnp.concatenate([core[30:34, 26:34], jnp.zeros((4, 18), F32)], 1)], 0
    )
    tail = jnp.concatenate([tail, jnp.zeros((2, 26), F32)], 0)
    groups = [core[10 * g : 10 * g + 10, 0:34] for g in range(3)]
    return jnp.concatenate([*groups, tail], 1)


def core_from_rows(both):
    top = jnp.concatenate([both[:, 34 * g : 34 * g + 34] for g in range(3)], 0)
    last = jnp.concatenate([both[0:4, 102:128], both[4:8, 102:110]], 1)
    core = jnp.concatenate([top, last, jnp.zeros((PAD - 34, 34), F32)], 0)
    return jnp.concatenate([core, jnp.zeros((PAD, PAD - 34), F32)], 1)


def core_kernel(log_targets):
    def body(arrived, features, former, packed, columns, total, *tiles):
        column_stack(arrived, columns, log_targets)
        total[...] = jnp.zeros_like(total)

        def consume(tile, b):
            width = tile.shape[1]
            stack = columns[:, pl.ds(pl.multiple_of(b * width, width), width)]
            plan = jnp.exp2(tile[...])
            high = plan.astype(BF16)
            low = (plan - high.astype(F32)).astype(BF16)
            total[...] += dot(high, stack, ((1,), (1,))) + dot(low, stack, ((1,), (1,)))

        in_turns(former, columns, consume, tiles)
        carried = (
            total[:, 0:PAD] + total[:, 2 * PAD : 3 * PAD] + total[:, 4 * PAD : 5 * PAD]
        )
        part = dot(features[...], carried, ((1,), (0,)), HIGHEST)
        part = jnp.concatenate([part[0:32], part[33:34], part[32:33]], 0)
        part = jnp.concatenate([part[:, 0:32], part[:, 33:34], part[:, 32:33]], 1)
        both = core_to_rows(part)
        for k in range(packed.shape[0] // 10):
            packed[10 * k : 10 * k + 10, :] = both

    return body


def row_kernel(parts, features, columns, out, core_out, core_new, former, highest, total, *tiles):
    core = core_from_rows(sum(parts[10 * k : 10 * k + 10, :] for k in range(parts.shape[0] // 10)))
    core_out[...] = core
    core_new[...] = turned_back(core)
    former[...] = former_stack(weighted_core(core, features[...]), None, 1.0)
    rows = features.shape[1]
    highest[...] = jnp.full(highest.shape, jnp.finfo(F32).min, F32)
    total[...] = jnp.zeros_like(total)

    def consume(tile, _):
        for r in range(0, rows, 64):
            at = pl.ds(r, 64)
            pieces = [tile[at, LANES * k : LANES * k + LANES] for k in range(tile.shape[1] // LANES)]
            before = highest[at, :]
            now = largest([before, *pieces])
            highest[at, :] = now
            total[at, :] = total[at, :] * jnp.exp2(before - now) + sum(
                jnp.exp2(p - now) for p in pieces
            )

    in_turns(former, columns, consume, tiles)
    lanes = highest[...]
    top = jnp.max(lanes, 1, keepdims=True)
    added = jnp.sum(total[...] * jnp.exp2(lanes - top), 1, keepdims=True)
    part = top * LN2 + jnp.log(added)
    wide = jnp.broadcast_to(part, (rows, LANES))
    flat = [jnp.transpose(wide[LANES * k : LANES * k + LANES])[0:1] for k in range(4)]
    both = jnp.concatenate(flat, 0)
    for k in range(out.shape[0] // 4):
        out[4 * k : 4 * k + 4, :] = both


def largest(values):
    return functools.reduce(jnp.maximum, values)


def combined(values):
    highest = largest(values)
    total = sum(jnp.exp(v - highest) for v in values)
    return highest + jnp.log(total)


def column_pieces(tile, b):
    count = tile.shape[1] // LANES
    return [(pl.ds(b * count + k, 1), tile[:, LANES * k : LANES * k + LANES]) for k in range(count)]


def in_lanes(rows):
    return jnp.concatenate([rows[k : k + 1] for k in range(rows.shape[0])], 1)


def ahead_kernel(own_parts, features, log_source, core, columns, weighted_out, bound, former, *tiles):
    weighted = weighted_core(core[...], features[...])
    weighted_out[...] = weighted
    term = 2.0 * log_source[...] - in_lanes(own_parts[0:4, :])
    former[...] = former_stack(weighted, term, 0.0)

    def consume(tile, b):
        for at, piece in column_pieces(tile, b):
            bound[at, :] = jnp.max(piece, 0, keepdims=True)

    in_turns(former, columns, consume, tiles)


def column_kernel(
    parts, log_source, weighted, bound, columns, own_out, out, former, sums, shift, mine, *tiles
):
    merged = in_lanes(combined([parts[4 * k : 4 * k + 4, :] for k in range(parts.shape[0] // 4)]))
    logs = log_source[...]
    source_new = EPSILON * (logs - merged)
    own = own_out.shape[1]
    for k in range(mine.shape[0]):
        mine[k : k + 1, :] = source_new[:, own * k : own * k + own]
    own_out[...] = mine[pl.ds(lax.axis_index("z"), 1), :]
    former[...] = former_stack(weighted[...], logs + source_new * (1.0 / EPSILON), 0.0)
    shift[...] = bound[...]

    def add(tile, b):
        for at, piece in column_pieces(tile, b):
            sums[at, :] = jnp.sum(jnp.exp2(piece - shift[at, :]), 0, keepdims=True)

    in_turns(former, columns, add, tiles)
    safe = jnp.min(sums[...]) >= FLOOR

    @pl.when(jnp.logical_not(safe))
    def _():
        def add_over_largest(tile, b):
            for at, piece in column_pieces(tile, b):
                highest = jnp.max(piece, 0, keepdims=True)
                shift[at, :] = highest
                sums[at, :] = jnp.sum(jnp.exp2(piece - highest), 0, keepdims=True)

        in_turns(former, columns, add_over_largest, tiles)

    part = shift[...] * LN2 + jnp.log(sums[...])
    for y in range(4):
        for s in range(8):
            at = 8 * (4 * s + y)
            out[at : at + 8, :] = part[8 * y : 8 * y + 8]


def last_kernel(log_targets):
    def body(parts, weight, out):
        merged = combined([parts[8 * k : 8 * k + 8, :] for k in range(parts.shape[0] // 8)])
        out[...] = EPSILON * (jnp.log(weight[...]) - log_targets - merged)

    return body


def on_device(
    source_points,
    target_points,
    source_potential,
    target_potential,
    source_weight,
    target_weight,
    core_previous,
):
    emb, own = source_points.shape
    dims, span = target_points.shape
    n_z, n_y, n_src = lax.axis_size("z"), lax.axis_size("y"), lax.axis_size(("x", "core"))
    n_plane = n_src * n_y
    rows, columns = own * n_z, span * n_y
    log_sources = math.log(own * n_z * n_plane)
    log_targets = math.log(span * n_z * n_y)
    given = (
        source_points,
        source_potential.reshape(1, own),
        source_weight.reshape(1, own),
        target_points,
        target_potential.reshape(8, LANES),
        target_weight.reshape(8, LANES),
        core_previous,
    )
    mine, theirs, previous = pl.pallas_call(
        pack,
        out_shape=(
            jax.ShapeDtypeStruct((9 * n_z, LANES), F32),
            jax.ShapeDtypeStruct((34 * n_plane, LANES), F32),
            jax.ShapeDtypeStruct((PAD, PAD), F32),
        ),
        in_specs=[pl.BlockSpec(memory_space=pltpu.HBM)] * len(given),
        out_specs=(VMEM, VMEM, VMEM),
        scratch_shapes=[
            pltpu.VMEM((PAD, LANES), F32),
            pltpu.SemaphoreType.DMA((len(given),)),
            *(pltpu.VMEM(a.shape, F32) for a in given),
        ],
        name="pack",
    )(*given)
    theirs = exchange(theirs.reshape(n_plane, 1, 34 * LANES), PLANE).reshape(-1, LANES)
    mine = exchange(mine.reshape(n_z, 1, 9 * LANES), "z").reshape(-1, LANES)
    former = pltpu.VMEM((DEPTH, rows), BF16)
    tiles = (pltpu.VMEM((rows, 512), F32), pltpu.VMEM((rows, 512), F32))
    features, log_source, core_former = call(
        source_kernel(log_sources),
        [((PAD, rows), F32), ((1, rows), F32), ((DEPTH, rows), BF16)],
        (mine, previous),
        name="sources",
    )
    packed, stack = call(
        core_kernel(log_targets),
        [((10 * n_plane, LANES), F32), ((DEPTH, columns), BF16)],
        (theirs, features, core_former),
        scratch=[pltpu.VMEM((rows, DEPTH), F32), *tiles],
        name="core",
        grant=16,
    )
    parts = exchange(packed.reshape(n_plane, 1, 10 * LANES), PLANE)
    parts = jnp.broadcast_to(jnp.sum(parts, 0, keepdims=True), (n_z, 1, 10 * LANES))
    parts = exchange(parts, "z").reshape(-1, LANES)

    per_lane = pltpu.VMEM((rows, LANES), F32)
    own_parts, core, core_new = call(
        row_kernel,
        [((4 * n_z, LANES), F32), ((PAD, PAD), F32), (core_previous.shape, F32)],
        (parts, features, stack),
        scratch=[former, per_lane, per_lane, *tiles],
        name="rows",
        grant=16,
    )
    row_parts = exchange(own_parts.reshape(n_z, 1, rows), "z").reshape(-1, LANES)
    per_column = (columns // LANES, LANES)
    weighted, bound = call(
        ahead_kernel,
        [((PAD, rows), F32), (per_column, F32)],
        (own_parts, features, log_source, core, stack),
        scratch=[former, *tiles],
        name="ahead",
        grant=16,
    )
    own_rows, column_parts = call(
        column_kernel,
        [((1, own), F32), ((8 * n_plane, LANES), F32)],
        (row_parts, log_source, weighted, bound, stack),
        scratch=[
            former,
            pltpu.VMEM(per_column, F32),
            pltpu.VMEM(per_column, F32),
            pltpu.VMEM((n_z, own), F32),
            *tiles,
        ],
        name="columns",
        grant=16,
    )
    column_parts = exchange(column_parts.reshape(n_plane, 1, span), PLANE).reshape(-1, LANES)
    (target_new,) = call(
        last_kernel(log_targets),
        [((8, LANES), F32)],
        (column_parts, target_weight.reshape(8, LANES)),
        name="last",
    )
    return (own_rows.reshape(own), target_new.reshape(span), core_new)


def solution(mesh):
    finer = Mesh(mesh.devices.reshape(4, 2, 4, 16), ALL)
    source, target = P(ALL), P(("y", "z"))
    placed = (
        P(None, ALL),
        P(("x", "core"), ("y", "z")),
        source,
        target,
        source,
        target,
        P(),
    )
    return jax.shard_map(
        on_device, mesh=finer, in_specs=placed, out_specs=(source, target, P()), check_vma=False
    )
```

```python
import functools
import math

import jax
import jax.numpy as jnp
from jax import lax
from jax.experimental import pallas as pl
from jax.experimental.pallas import tpu as pltpu
from jax.sharding import Mesh
from jax.sharding import PartitionSpec as P

PLANE = ("x", "core", "y")
ALL = ("x", "core", "y", "z")
EPSILON = 0.5
HIGHEST = lax.Precision.HIGHEST
LANES = 128
PAD = 40
DEPTH = 256
LOG2E = math.log2(math.e)
LN2 = math.log(2.0)
F32, BF16 = jnp.float32, jnp.bfloat16
VMEM = pl.BlockSpec(memory_space=pltpu.VMEM)


def call(body, outs, args, scratch=(), name=None, grant=8):
    return pl.pallas_call(
        body,
        out_shape=tuple(jax.ShapeDtypeStruct(s, d) for s, d in outs),
        in_specs=[VMEM] * len(args),
        out_specs=tuple(VMEM for _ in outs),
        scratch_shapes=list(scratch),
        compiler_params=pltpu.CompilerParams(vmem_limit_bytes=grant * 2**20),
        name=name,
    )(*args)


def exchange(copies, axis):
    return lax.all_to_all(copies, axis, split_axis=0, concat_axis=0, tiled=True)


def dot(former, latter, dims, precision=None):
    return lax.dot_general(
        former, latter, (dims, ((), ())), precision=precision, preferred_element_type=F32
    )


def split(value):
    first = value.astype(BF16).astype(F32)
    rest = value - first
    second = rest.astype(BF16).astype(F32)
    return first, second, rest - second


def stacked(pieces, order):
    blocks = [pieces[k] for k in order]
    filler = jnp.zeros((DEPTH - PAD * len(order), pieces[0].shape[1]), F32)
    return jnp.concatenate([*blocks, filler], 0).astype(BF16)


LATTER_ORDER = (0, 0, 1, 0, 2, 1)
FORMER_ORDER = (0, 1, 0, 2, 0, 1)


def pack(*refs):
    given, (out, column_out), (held, sem, *into) = refs[:7], refs[7:9], refs[9:]
    copies = [pltpu.make_async_copy(a, b, sem.at[k]) for k, (a, b) in enumerate(zip(given, into))]
    for copy in copies:
        copy.start()
    for copy in copies:
        copy.wait()
    points, potential, weight, column_points, column_potential, column_weight, core = into
    value = points[...]
    block = jnp.concatenate([value[8 * k : 8 * k + 8] for k in range(4)], axis=1)
    last = jnp.concatenate(
        [potential[...], weight[...], jnp.ones((1, LANES - 64), F32)], axis=1
    )
    held[0:34, 0:34] = core[...]
    z = lax.axis_index("z")
    share = [held[pl.ds(z + 16 * g, 1), 0:34] for g in range(3)]
    share = jnp.concatenate([*share, jnp.zeros((1, LANES - 3 * 34), F32)], 1)
    both = jnp.concatenate([block, last, share], 0)
    for k in range(out.shape[0] // 10):
        out[10 * k : 10 * k + 10, :] = both
    for r in range(4):
        for k in range(8):
            held[8 * r + k : 8 * r + k + 1, :] = column_points[
                r : r + 1, LANES * k : LANES * k + LANES
            ]
    src = lax.axis_index(("x", "core"))
    held[32:33, :] = column_potential[pl.ds(src, 1), :]
    held[33:34, :] = column_weight[pl.ds(src, 1), :]
    both = held[0:34, :]
    for k in range(column_out.shape[0] // 34):
        column_out[34 * k : 34 * k + 34, :] = both


def column_stack(message, out, y, log_targets):
    for k in range(8):
        points = jnp.concatenate(
            [message[pl.ds(34 * (4 * s + y) + k, 4, stride=8), :] for s in range(8)], 0
        )
        squares = jnp.sum(points * points, 0, keepdims=True)
        at = 34 * (4 * k + y) + 32
        offset = jnp.log(message[pl.ds(at + 1, 1), :]) - log_targets
        offset = (offset + message[pl.ds(at, 1), :] * (1.0 / EPSILON)) * LOG2E
        tail = jnp.concatenate(
            [squares, jnp.ones((1, LANES), F32), offset, jnp.zeros((5, LANES), F32)], 0
        )
        value = jnp.concatenate([points, tail], 0)
        col = pl.multiple_of(1024 * y + LANES * k, LANES)
        out[:, pl.ds(col, LANES)] = stacked(split(value), LATTER_ORDER)


def in_turns(former, columns, consume, tiles, prepare=None):
    count = len(tiles)
    lead = count // 2
    width = tiles[0].shape[1]
    blocks = columns.shape[1] // width

    def fill(k, b):
        at = pl.multiple_of(jnp.minimum(b, blocks - 1) * width, width)
        tiles[k][...] = dot(former[...], columns[:, pl.ds(at, width)], ((0,), (0,)))

    for k in range(lead):
        fill(k, k)

    def step(i, _):
        for k in range(count):
            if prepare and k == count // 2:
                prepare(i + 1)
            fill((k + lead) % count, count * i + k + lead)
            consume(tiles[k], count * i + k)
        return 0

    lax.fori_loop(0, blocks // count, step, 0)


def signs(core):
    row = lax.broadcasted_iota(jnp.int32, core.shape, 0)
    col = lax.broadcasted_iota(jnp.int32, core.shape, 1)
    core = jnp.where(row < 32, -2.0 * core, core)
    return jnp.where(col < 32, -2.0 * core, core)


def weighted_core(core, features):
    return dot(signs(core), features, ((0,), (0,)), HIGHEST) * (2.0 / EPSILON * LOG2E)


def former_stack(weighted, row_term, column_factor):
    row = lax.broadcasted_iota(jnp.int32, weighted.shape, 0)
    if row_term is not None:
        weighted = jnp.where(row == 33, weighted + row_term * LOG2E, weighted)
    weighted = jnp.where(row == 34, column_factor, weighted)
    return stacked(split(weighted), FORMER_ORDER)


def turned(core):
    core = jnp.concatenate([core[2:34], core[0:2], jnp.zeros((PAD - 34, 34), F32)], 0)
    return jnp.concatenate([core[:, 2:34], core[:, 0:2], jnp.zeros((PAD, PAD - 34), F32)], 1)


def turned_back(core):
    core = jnp.concatenate([core[32:34], core[0:32]], 0)
    return jnp.concatenate([core[:, 32:34], core[:, 0:32]], 1)


def unpacked_sources(message, log_sources):
    pieces = []
    for k in range(4):
        pieces.append(
            jnp.concatenate(
                [message[10 * z : 10 * z + 8, 32 * k : 32 * k + 32] for z in range(16)], 1
            )
        )
    points = jnp.concatenate(pieces, 0)
    last = jnp.concatenate([message[10 * z + 8 : 10 * z + 9, 0:32] for z in range(16)], 1)
    weight = jnp.concatenate([message[10 * z + 8 : 10 * z + 9, 32:64] for z in range(16)], 1)
    squares = jnp.sum(points * points, 0, keepdims=True)
    zeros = jnp.zeros((6, squares.shape[1]), F32)
    features = jnp.concatenate([points, squares, jnp.ones_like(squares), zeros], 0)
    shares = message[pl.ds(9, 16, stride=10), :]
    core = jnp.concatenate([shares[:, 34 * g : 34 * g + 34] for g in range(3)], 0)
    return features, jnp.log(weight) - log_sources, last, turned(core)


def core_to_rows(core):
    tail = jnp.concatenate(
        [core[30:34, 0:26], jnp.concatenate([core[30:34, 26:34], jnp.zeros((4, 18), F32)], 1)], 0
    )
    tail = jnp.concatenate([tail, jnp.zeros((2, 26), F32)], 0)
    groups = [core[10 * g : 10 * g + 10, 0:34] for g in range(3)]
    return jnp.concatenate([*groups, tail], 1)


def core_from_rows(both):
    top = jnp.concatenate([both[:, 34 * g : 34 * g + 34] for g in range(3)], 0)
    last = jnp.concatenate([both[0:4, 102:128], both[4:8, 102:110]], 1)
    core = jnp.concatenate([top, last, jnp.zeros((PAD - 34, 34), F32)], 0)
    return jnp.concatenate([core, jnp.zeros((PAD, PAD - 34), F32)], 1)


def core_kernel(log_sources, log_targets):
    def body(message, arrived, packed, columns, features, log_out, former, total, *tiles):
        value, log_source, potential, core = unpacked_sources(message, log_sources)
        features[...] = value
        log_out[...] = log_source
        former[...] = former_stack(
            weighted_core(core, value), log_source + potential * (1.0 / EPSILON), 1.0
        )
        total[...] = jnp.zeros_like(total)

        def prepare(y):
            column_stack(arrived, columns, jnp.minimum(y, 3), log_targets)

        prepare(0)

        def consume(tile, b):
            width = tile.shape[1]
            stack = columns[:, pl.ds(pl.multiple_of(b * width, width), width)]
            plan = jnp.exp2(tile[...])
            high = plan.astype(BF16)
            low = (plan - high.astype(F32)).astype(BF16)
            total[...] += dot(high, stack, ((1,), (1,))) + dot(low, stack, ((1,), (1,)))

        in_turns(former, columns, consume, tiles, prepare)
        carried = (
            total[:, 0:PAD] + total[:, 2 * PAD : 3 * PAD] + total[:, 4 * PAD : 5 * PAD]
        )
        part = dot(features[...], carried, ((1,), (0,)), HIGHEST)
        part = jnp.concatenate([part[0:32], part[33:34], part[32:33]], 0)
        part = jnp.concatenate([part[:, 0:32], part[:, 33:34], part[:, 32:33]], 1)
        both = core_to_rows(part)
        for k in range(packed.shape[0] // 10):
            packed[10 * k : 10 * k + 10, :] = both

    return body


def row_kernel(parts, features, columns, out, core_out, former, highest, total, *tiles):
    core = core_from_rows(sum(parts[10 * k : 10 * k + 10, :] for k in range(parts.shape[0] // 10)))
    core_out[...] = core
    former[...] = former_stack(weighted_core(core, features[...]), None, 1.0)
    rows = features.shape[1]
    highest[...] = jnp.full(highest.shape, jnp.finfo(F32).min, F32)
    total[...] = jnp.zeros_like(total)

    def consume(tile, _):
        for r in range(0, rows, 64):
            at = pl.ds(r, 64)
            pieces = [tile[at, LANES * k : LANES * k + LANES] for k in range(tile.shape[1] // LANES)]
            before = highest[at, :]
            now = largest([before, *pieces])
            highest[at, :] = now
            total[at, :] = total[at, :] * jnp.exp2(before - now) + sum(
                jnp.exp2(p - now) for p in pieces
            )

    in_turns(former, columns, consume, tiles)
    lanes = highest[...]
    top = jnp.max(lanes, 1, keepdims=True)
    added = jnp.sum(total[...] * jnp.exp2(lanes - top), 1, keepdims=True)
    part = top * LN2 + jnp.log(added)
    wide = jnp.broadcast_to(part, (rows, LANES))
    flat = [jnp.transpose(wide[LANES * k : LANES * k + LANES])[0:1] for k in range(4)]
    both = jnp.concatenate(flat, 0)
    for k in range(out.shape[0] // 4):
        out[4 * k : 4 * k + 4, :] = both


def largest(values):
    return functools.reduce(jnp.maximum, values)


def combined(values):
    highest = largest(values)
    total = sum(jnp.exp(v - highest) for v in values)
    return highest + jnp.log(total)


def column_pieces(tile, b):
    count = tile.shape[1] // LANES
    return [(pl.ds(b * count + k, 1), tile[:, LANES * k : LANES * k + LANES]) for k in range(count)]


def in_lanes(rows):
    return jnp.concatenate([rows[k : k + 1] for k in range(rows.shape[0])], 1)


def column_kernel(
    parts, log_source, features, core, columns, own_out, out, former, held, mine, *tiles
):
    merged = in_lanes(combined([parts[4 * k : 4 * k + 4, :] for k in range(parts.shape[0] // 4)]))
    logs = log_source[...]
    source_new = EPSILON * (logs - merged)
    own = own_out.shape[1]
    for k in range(mine.shape[0]):
        mine[k : k + 1, :] = source_new[:, own * k : own * k + own]
    own_out[...] = mine[pl.ds(lax.axis_index("z"), 1), :]
    weighted = weighted_core(core[...], features[...])
    former[...] = former_stack(weighted, logs + source_new * (1.0 / EPSILON), 0.0)

    def consume(tile, b):
        for at, piece in column_pieces(tile, b):
            highest = jnp.max(piece, 0, keepdims=True)
            total = jnp.sum(jnp.exp2(piece - highest), 0, keepdims=True)
            held[at, :] = highest * LN2 + jnp.log(total)

    in_turns(former, columns, consume, tiles)
    for y in range(4):
        piece = held[8 * y : 8 * y + 8, :]
        for s in range(8):
            at = 8 * (4 * s + y)
            out[at : at + 8, :] = piece


def last_kernel(log_targets):
    def body(parts, weight, own_rows, core, out, own_out, core_out):
        own_out[...] = own_rows[...]
        core_out[...] = turned_back(core[...])
        merged = combined([parts[8 * k : 8 * k + 8, :] for k in range(parts.shape[0] // 8)])
        out[...] = EPSILON * (jnp.log(weight[...]) - log_targets - merged)

    return body


def on_device(
    source_points,
    target_points,
    source_potential,
    target_potential,
    source_weight,
    target_weight,
    core_previous,
):
    emb, own = source_points.shape
    dims, span = target_points.shape
    n_z, n_y, n_src = lax.axis_size("z"), lax.axis_size("y"), lax.axis_size(("x", "core"))
    n_plane = n_src * n_y
    rows, columns = own * n_z, span * n_y
    log_sources = math.log(own * n_z * n_plane)
    log_targets = math.log(span * n_z * n_y)
    given = (
        source_points,
        source_potential.reshape(1, own),
        source_weight.reshape(1, own),
        target_points,
        target_potential.reshape(8, LANES),
        target_weight.reshape(8, LANES),
        core_previous,
    )
    mine, theirs = pl.pallas_call(
        pack,
        out_shape=(
            jax.ShapeDtypeStruct((10 * n_z, LANES), F32),
            jax.ShapeDtypeStruct((34 * n_plane, LANES), F32),
        ),
        in_specs=[pl.BlockSpec(memory_space=pltpu.HBM)] * len(given),
        out_specs=(VMEM, VMEM),
        scratch_shapes=[
            pltpu.VMEM((48, LANES), F32),
            pltpu.SemaphoreType.DMA((len(given),)),
            *(pltpu.VMEM(a.shape, F32) for a in given),
        ],
        name="pack",
    )(*given)
    theirs = exchange(theirs.reshape(n_plane, 1, 34 * LANES), PLANE).reshape(-1, LANES)
    mine = exchange(mine.reshape(n_z, 1, 10 * LANES), "z").reshape(-1, LANES)
    former = pltpu.VMEM((DEPTH, rows), BF16)
    tile = pltpu.VMEM((rows, 512), F32)
    packed, stack, features, log_source = call(
        core_kernel(log_sources, log_targets),
        [
            ((10 * n_plane, LANES), F32),
            ((DEPTH, columns), BF16),
            ((PAD, rows), F32),
            ((1, rows), F32),
        ],
        (mine, theirs),
        scratch=[former, pltpu.VMEM((rows, DEPTH), F32), tile, tile],
        name="core",
        grant=16,
    )
    parts = exchange(packed.reshape(n_plane, 1, 10 * LANES), PLANE)
    parts = jnp.broadcast_to(jnp.sum(parts, 0, keepdims=True), (n_z, 1, 10 * LANES))
    parts = exchange(parts, "z").reshape(-1, LANES)

    per_lane = pltpu.VMEM((rows, LANES), F32)
    row_parts, core = call(
        row_kernel,
        [((4 * n_z, LANES), F32), ((PAD, PAD), F32)],
        (parts, features, stack),
        scratch=[former, per_lane, per_lane, tile, tile, tile, tile],
        name="rows",
        grant=16,
    )
    row_parts = exchange(row_parts.reshape(n_z, 1, rows), "z").reshape(-1, LANES)
    own_rows, column_parts = call(
        column_kernel,
        [((1, own), F32), ((8 * n_plane, LANES), F32)],
        (row_parts, log_source, features, core, stack),
        scratch=[
            former,
            pltpu.VMEM((columns // LANES, LANES), F32),
            pltpu.VMEM((n_z, own), F32),
            *(tile, tile, tile, tile),
        ],
        name="columns",
        grant=16,
    )
    column_parts = exchange(column_parts.reshape(n_plane, 1, span), PLANE).reshape(-1, LANES)
    target_new, own_rows, core_new = call(
        last_kernel(log_targets),
        [((8, LANES), F32), ((1, own), F32), (core_previous.shape, F32)],
        (column_parts, target_weight.reshape(8, LANES), own_rows, core),
        name="last",
    )
    return (own_rows.reshape(own), target_new.reshape(span), core_new)


def solution(mesh):
    finer = Mesh(mesh.devices.reshape(4, 2, 4, 16), ALL)
    source, target = P(ALL), P(("y", "z"))
    placed = (
        P(None, ALL),
        P(("x", "core"), ("y", "z")),
        source,
        target,
        source,
        target,
        P(),
    )
    return jax.shard_map(
        on_device, mesh=finer, in_specs=placed, out_specs=(source, target, P()), check_vma=False
    )
```

```python
import functools
import math

import jax
import jax.numpy as jnp
from jax import lax
from jax.experimental import pallas as pl
from jax.experimental.pallas import tpu as pltpu
from jax.sharding import Mesh
from jax.sharding import PartitionSpec as P

PLANE = ("x", "core", "y")
ALL = ("x", "core", "y", "z")
EPSILON = 0.5
HIGHEST = lax.Precision.HIGHEST
LANES = 128
PAD = 40
DEPTH = 256
LOG2E = math.log2(math.e)
LN2 = math.log(2.0)
F32, BF16 = jnp.float32, jnp.bfloat16
VMEM = pl.BlockSpec(memory_space=pltpu.VMEM)


def call(body, outs, args, scratch=(), name=None, grant=8):
    return pl.pallas_call(
        body,
        out_shape=tuple(jax.ShapeDtypeStruct(s, d) for s, d in outs),
        in_specs=[VMEM] * len(args),
        out_specs=tuple(VMEM for _ in outs),
        scratch_shapes=list(scratch),
        compiler_params=pltpu.CompilerParams(vmem_limit_bytes=grant * 2**20),
        name=name,
    )(*args)


def exchange(copies, axis):
    return lax.all_to_all(copies, axis, split_axis=0, concat_axis=0, tiled=True)


def dot(former, latter, dims, precision=None):
    return lax.dot_general(
        former, latter, (dims, ((), ())), precision=precision, preferred_element_type=F32
    )


def split(value):
    first = value.astype(BF16).astype(F32)
    rest = value - first
    second = rest.astype(BF16).astype(F32)
    return first, second, rest - second


def stacked(pieces, order):
    blocks = [pieces[k] for k in order]
    filler = jnp.zeros((DEPTH - PAD * len(order), pieces[0].shape[1]), F32)
    return jnp.concatenate([*blocks, filler], 0).astype(BF16)


LATTER_ORDER = (0, 0, 1, 0, 2, 1)
FORMER_ORDER = (0, 1, 0, 2, 0, 1)


def pack(*refs):
    given, (out, column_out), (held, sem, *into) = refs[:7], refs[7:9], refs[9:]
    copies = [pltpu.make_async_copy(a, b, sem.at[k]) for k, (a, b) in enumerate(zip(given, into))]
    for copy in copies:
        copy.start()
    for copy in copies:
        copy.wait()
    points, potential, weight, column_points, column_potential, column_weight, core = into
    value = points[...]
    block = jnp.concatenate([value[8 * k : 8 * k + 8] for k in range(4)], axis=1)
    last = jnp.concatenate(
        [potential[...], weight[...], jnp.ones((1, LANES - 64), F32)], axis=1
    )
    held[0:34, 0:34] = core[...]
    z = lax.axis_index("z")
    share = [held[pl.ds(z + 16 * g, 1), 0:34] for g in range(3)]
    share = jnp.concatenate([*share, jnp.zeros((1, LANES - 3 * 34), F32)], 1)
    both = jnp.concatenate([block, last, share], 0)
    for k in range(out.shape[0] // 10):
        out[10 * k : 10 * k + 10, :] = both
    for r in range(4):
        for k in range(8):
            held[8 * r + k : 8 * r + k + 1, :] = column_points[
                r : r + 1, LANES * k : LANES * k + LANES
            ]
    src = lax.axis_index(("x", "core"))
    held[32:33, :] = column_potential[pl.ds(src, 1), :]
    held[33:34, :] = column_weight[pl.ds(src, 1), :]
    both = held[0:34, :]
    for k in range(column_out.shape[0] // 34):
        column_out[34 * k : 34 * k + 34, :] = both


def column_stack(message, out, y, log_targets):
    for k in range(8):
        points = jnp.concatenate(
            [message[pl.ds(34 * (4 * s + y) + k, 4, stride=8), :] for s in range(8)], 0
        )
        squares = jnp.sum(points * points, 0, keepdims=True)
        at = 34 * (4 * k + y) + 32
        offset = jnp.log(message[pl.ds(at + 1, 1), :]) - log_targets
        offset = (offset + message[pl.ds(at, 1), :] * (1.0 / EPSILON)) * LOG2E
        tail = jnp.concatenate(
            [squares, jnp.ones((1, LANES), F32), offset, jnp.zeros((5, LANES), F32)], 0
        )
        value = jnp.concatenate([points, tail], 0)
        col = pl.multiple_of(1024 * y + LANES * k, LANES)
        out[:, pl.ds(col, LANES)] = stacked(split(value), LATTER_ORDER)


def in_turns(former, columns, consume, tiles, prepare=None):
    count = len(tiles)
    lead = count // 2
    width = tiles[0].shape[1]
    blocks = columns.shape[1] // width

    def fill(k, b):
        at = pl.multiple_of(jnp.minimum(b, blocks - 1) * width, width)
        tiles[k][...] = dot(former[...], columns[:, pl.ds(at, width)], ((0,), (0,)))

    for k in range(lead):
        fill(k, k)

    def step(i, _):
        for k in range(count):
            if prepare and k == count // 2:
                prepare(i + 1)
            fill((k + lead) % count, count * i + k + lead)
            consume(tiles[k], count * i + k)
        return 0

    lax.fori_loop(0, blocks // count, step, 0)


def signs(core):
    row = lax.broadcasted_iota(jnp.int32, core.shape, 0)
    col = lax.broadcasted_iota(jnp.int32, core.shape, 1)
    core = jnp.where(row < 32, -2.0 * core, core)
    return jnp.where(col < 32, -2.0 * core, core)


def weighted_core(core, features):
    return dot(signs(core), features, ((0,), (0,)), HIGHEST) * (2.0 / EPSILON * LOG2E)


def former_stack(weighted, row_term, column_factor):
    row = lax.broadcasted_iota(jnp.int32, weighted.shape, 0)
    if row_term is not None:
        weighted = jnp.where(row == 33, weighted + row_term * LOG2E, weighted)
    weighted = jnp.where(row == 34, column_factor, weighted)
    return stacked(split(weighted), FORMER_ORDER)


def turned(core):
    core = jnp.concatenate([core[2:34], core[0:2], jnp.zeros((PAD - 34, 34), F32)], 0)
    return jnp.concatenate([core[:, 2:34], core[:, 0:2], jnp.zeros((PAD, PAD - 34), F32)], 1)


def turned_back(core):
    core = jnp.concatenate([core[32:34], core[0:32]], 0)
    return jnp.concatenate([core[:, 32:34], core[:, 0:32]], 1)


def unpacked_sources(message, log_sources):
    pieces = []
    for k in range(4):
        pieces.append(
            jnp.concatenate(
                [message[10 * z : 10 * z + 8, 32 * k : 32 * k + 32] for z in range(16)], 1
            )
        )
    points = jnp.concatenate(pieces, 0)
    last = jnp.concatenate([message[10 * z + 8 : 10 * z + 9, 0:32] for z in range(16)], 1)
    weight = jnp.concatenate([message[10 * z + 8 : 10 * z + 9, 32:64] for z in range(16)], 1)
    squares = jnp.sum(points * points, 0, keepdims=True)
    zeros = jnp.zeros((6, squares.shape[1]), F32)
    features = jnp.concatenate([points, squares, jnp.ones_like(squares), zeros], 0)
    shares = message[pl.ds(9, 16, stride=10), :]
    core = jnp.concatenate([shares[:, 34 * g : 34 * g + 34] for g in range(3)], 0)
    return features, jnp.log(weight) - log_sources, last, turned(core)


def core_to_rows(core):
    tail = jnp.concatenate(
        [core[30:34, 0:26], jnp.concatenate([core[30:34, 26:34], jnp.zeros((4, 18), F32)], 1)], 0
    )
    tail = jnp.concatenate([tail, jnp.zeros((2, 26), F32)], 0)
    groups = [core[10 * g : 10 * g + 10, 0:34] for g in range(3)]
    return jnp.concatenate([*groups, tail], 1)


def core_from_rows(both):
    top = jnp.concatenate([both[:, 34 * g : 34 * g + 34] for g in range(3)], 0)
    last = jnp.concatenate([both[0:4, 102:128], both[4:8, 102:110]], 1)
    core = jnp.concatenate([top, last, jnp.zeros((PAD - 34, 34), F32)], 0)
    return jnp.concatenate([core, jnp.zeros((PAD, PAD - 34), F32)], 1)


def core_kernel(log_sources, log_targets):
    def body(message, arrived, packed, columns, features, log_out, former, total, *tiles):
        value, log_source, potential, core = unpacked_sources(message, log_sources)
        features[...] = value
        log_out[...] = log_source
        former[...] = former_stack(
            weighted_core(core, value), log_source + potential * (1.0 / EPSILON), 1.0
        )
        total[...] = jnp.zeros_like(total)

        def prepare(y):
            column_stack(arrived, columns, jnp.minimum(y, 3), log_targets)

        prepare(0)

        def consume(tile, b):
            width = tile.shape[1]
            stack = columns[:, pl.ds(pl.multiple_of(b * width, width), width)]
            plan = jnp.exp2(tile[...])
            high = plan.astype(BF16)
            low = (plan - high.astype(F32)).astype(BF16)
            total[...] += dot(high, stack, ((1,), (1,))) + dot(low, stack, ((1,), (1,)))

        in_turns(former, columns, consume, tiles, prepare)
        carried = (
            total[:, 0:PAD] + total[:, 2 * PAD : 3 * PAD] + total[:, 4 * PAD : 5 * PAD]
        )
        part = dot(features[...], carried, ((1,), (0,)), HIGHEST)
        part = jnp.concatenate([part[0:32], part[33:34], part[32:33]], 0)
        part = jnp.concatenate([part[:, 0:32], part[:, 33:34], part[:, 32:33]], 1)
        both = core_to_rows(part)
        for k in range(packed.shape[0] // 10):
            packed[10 * k : 10 * k + 10, :] = both

    return body


def row_kernel(parts, features, columns, out, core_out, former, highest, total, *tiles):
    core = core_from_rows(sum(parts[10 * k : 10 * k + 10, :] for k in range(parts.shape[0] // 10)))
    core_out[...] = core
    former[...] = former_stack(weighted_core(core, features[...]), None, 1.0)
    rows = features.shape[1]
    highest[...] = jnp.full(highest.shape, jnp.finfo(F32).min, F32)
    total[...] = jnp.zeros_like(total)

    def consume(tile, _):
        for r in range(0, rows, 64):
            at = pl.ds(r, 64)
            pieces = [tile[at, LANES * k : LANES * k + LANES] for k in range(tile.shape[1] // LANES)]
            before = highest[at, :]
            now = largest([before, *pieces])
            highest[at, :] = now
            total[at, :] = total[at, :] * jnp.exp2(before - now) + sum(
                jnp.exp2(p - now) for p in pieces
            )

    in_turns(former, columns, consume, tiles)
    lanes = highest[...]
    top = jnp.max(lanes, 1, keepdims=True)
    added = jnp.sum(total[...] * jnp.exp2(lanes - top), 1, keepdims=True)
    part = top * LN2 + jnp.log(added)
    wide = jnp.broadcast_to(part, (rows, LANES))
    flat = [jnp.transpose(wide[LANES * k : LANES * k + LANES])[0:1] for k in range(4)]
    both = jnp.concatenate(flat, 0)
    for k in range(out.shape[0] // 4):
        out[4 * k : 4 * k + 4, :] = both


def largest(values):
    return functools.reduce(jnp.maximum, values)


def combined(values):
    highest = largest(values)
    total = sum(jnp.exp(v - highest) for v in values)
    return highest + jnp.log(total)


def column_pieces(tile, b):
    count = tile.shape[1] // LANES
    return [(pl.ds(b * count + k, 1), tile[:, LANES * k : LANES * k + LANES]) for k in range(count)]


def in_lanes(rows):
    return jnp.concatenate([rows[k : k + 1] for k in range(rows.shape[0])], 1)


def column_kernel(
    parts, log_source, features, core, columns, own_out, out, former, held, mine, *tiles
):
    merged = in_lanes(combined([parts[4 * k : 4 * k + 4, :] for k in range(parts.shape[0] // 4)]))
    logs = log_source[...]
    source_new = EPSILON * (logs - merged)
    own = own_out.shape[1]
    for k in range(mine.shape[0]):
        mine[k : k + 1, :] = source_new[:, own * k : own * k + own]
    own_out[...] = mine[pl.ds(lax.axis_index("z"), 1), :]
    weighted = weighted_core(core[...], features[...])
    former[...] = former_stack(weighted, logs + source_new * (1.0 / EPSILON), 0.0)

    def consume(tile, b):
        for at, piece in column_pieces(tile, b):
            highest = jnp.max(piece, 0, keepdims=True)
            total = jnp.sum(jnp.exp2(piece - highest), 0, keepdims=True)
            held[at, :] = highest * LN2 + jnp.log(total)

    in_turns(former, columns, consume, tiles)
    for y in range(4):
        piece = held[8 * y : 8 * y + 8, :]
        for s in range(8):
            at = 8 * (4 * s + y)
            out[at : at + 8, :] = piece


def last_kernel(log_targets):
    def body(parts, weight, own_rows, core, out, own_out, core_out):
        own_out[...] = own_rows[...]
        core_out[...] = turned_back(core[...])
        merged = combined([parts[8 * k : 8 * k + 8, :] for k in range(parts.shape[0] // 8)])
        out[...] = EPSILON * (jnp.log(weight[...]) - log_targets - merged)

    return body


def on_device(
    source_points,
    target_points,
    source_potential,
    target_potential,
    source_weight,
    target_weight,
    core_previous,
):
    emb, own = source_points.shape
    dims, span = target_points.shape
    n_z, n_y, n_src = lax.axis_size("z"), lax.axis_size("y"), lax.axis_size(("x", "core"))
    n_plane = n_src * n_y
    rows, columns = own * n_z, span * n_y
    log_sources = math.log(own * n_z * n_plane)
    log_targets = math.log(span * n_z * n_y)
    given = (
        source_points,
        source_potential.reshape(1, own),
        source_weight.reshape(1, own),
        target_points,
        target_potential.reshape(8, LANES),
        target_weight.reshape(8, LANES),
        core_previous,
    )
    mine, theirs = pl.pallas_call(
        pack,
        out_shape=(
            pltpu.VMEM((10 * n_z, LANES), F32),
            pltpu.VMEM((34 * n_plane, LANES), F32),
        ),
        in_specs=[pl.BlockSpec(memory_space=pltpu.HBM)] * len(given),
        out_specs=(VMEM, VMEM),
        scratch_shapes=[
            pltpu.VMEM((48, LANES), F32),
            pltpu.SemaphoreType.DMA((len(given),)),
            *(pltpu.VMEM(a.shape, F32) for a in given),
        ],
        compiler_params=pltpu.CompilerParams(vmem_limit_bytes=16 * 2**20),
        name="pack",
    )(*(pltpu.with_memory_space_constraint(a, pltpu.HBM) for a in given))
    theirs = exchange(theirs.reshape(n_plane, 1, 34 * LANES), PLANE).reshape(-1, LANES)
    mine = exchange(mine.reshape(n_z, 1, 10 * LANES), "z").reshape(-1, LANES)
    former = pltpu.VMEM((DEPTH, rows), BF16)
    tile = pltpu.VMEM((rows, 512), F32)
    packed, stack, features, log_source = call(
        core_kernel(log_sources, log_targets),
        [
            ((10 * n_plane, LANES), F32),
            ((DEPTH, columns), BF16),
            ((PAD, rows), F32),
            ((1, rows), F32),
        ],
        (mine, theirs),
        scratch=[former, pltpu.VMEM((rows, DEPTH), F32), tile, tile],
        name="core",
        grant=16,
    )
    parts = exchange(packed.reshape(n_plane, 1, 10 * LANES), PLANE)
    parts = jnp.broadcast_to(jnp.sum(parts, 0, keepdims=True), (n_z, 1, 10 * LANES))
    parts = exchange(parts, "z").reshape(-1, LANES)

    per_lane = pltpu.VMEM((rows, LANES), F32)
    row_parts, core = call(
        row_kernel,
        [((4 * n_z, LANES), F32), ((PAD, PAD), F32)],
        (parts, features, stack),
        scratch=[former, per_lane, per_lane, tile, tile, tile, tile],
        name="rows",
        grant=16,
    )
    row_parts = exchange(row_parts.reshape(n_z, 1, rows), "z").reshape(-1, LANES)
    own_rows, column_parts = call(
        column_kernel,
        [((1, own), F32), ((8 * n_plane, LANES), F32)],
        (row_parts, log_source, features, core, stack),
        scratch=[
            former,
            pltpu.VMEM((columns // LANES, LANES), F32),
            pltpu.VMEM((n_z, own), F32),
            *(tile, tile, tile, tile),
        ],
        name="columns",
        grant=16,
    )
    column_parts = exchange(column_parts.reshape(n_plane, 1, span), PLANE).reshape(-1, LANES)
    target_new, own_rows, core_new = call(
        last_kernel(log_targets),
        [((8, LANES), F32), ((1, own), F32), (core_previous.shape, F32)],
        (column_parts, target_weight.reshape(8, LANES), own_rows, core),
        name="last",
    )
    return (own_rows.reshape(own), target_new.reshape(span), core_new)


def solution(mesh):
    finer = Mesh(mesh.devices.reshape(4, 2, 4, 16), ALL)
    source, target = P(ALL), P(("y", "z"))
    placed = (
        P(None, ALL),
        P(("x", "core"), ("y", "z")),
        source,
        target,
        source,
        target,
        P(),
    )
    return jax.shard_map(
        on_device, mesh=finer, in_specs=placed, out_specs=(source, target, P()), check_vma=False
    )
```

```python
import functools
import math

import jax
import jax.numpy as jnp
from jax import lax
from jax.experimental import pallas as pl
from jax.experimental.pallas import tpu as pltpu
from jax.sharding import Mesh
from jax.sharding import PartitionSpec as P

PLANE = ("x", "core", "y")
ALL = ("x", "core", "y", "z")
EPSILON = 0.5
HIGHEST = lax.Precision.HIGHEST
LANES = 128
PAD = 40
DEPTH = 256
LOG2E = math.log2(math.e)
LN2 = math.log(2.0)
FLOOR = 2.0**-70
LIFT = 12.0
F32, BF16 = jnp.float32, jnp.bfloat16
VMEM = pl.BlockSpec(memory_space=pltpu.VMEM)


def call(body, outs, args, scratch=(), name=None, grant=8):
    return pl.pallas_call(
        body,
        out_shape=tuple(jax.ShapeDtypeStruct(s, d) for s, d in outs),
        in_specs=[VMEM] * len(args),
        out_specs=tuple(VMEM for _ in outs),
        scratch_shapes=list(scratch),
        compiler_params=pltpu.CompilerParams(vmem_limit_bytes=grant * 2**20),
        name=name,
    )(*args)


def exchange(copies, axis):
    return lax.all_to_all(copies, axis, split_axis=0, concat_axis=0, tiled=True)


def dot(former, latter, dims, precision=None):
    return lax.dot_general(
        former, latter, (dims, ((), ())), precision=precision, preferred_element_type=F32
    )


def split(value):
    first = value.astype(BF16).astype(F32)
    rest = value - first
    second = rest.astype(BF16).astype(F32)
    return first, second, rest - second


def stacked(pieces, order):
    blocks = [pieces[k] for k in order]
    filler = jnp.zeros((DEPTH - PAD * len(order), pieces[0].shape[1]), F32)
    return jnp.concatenate([*blocks, filler], 0).astype(BF16)


LATTER_ORDER = (0, 0, 1, 0, 2, 1)
FORMER_ORDER = (0, 1, 0, 2, 0, 1)


def pack(*refs):
    given, (out, column_out), (held, sem, *into) = refs[:7], refs[7:9], refs[9:]
    copies = [pltpu.make_async_copy(a, b, sem.at[k]) for k, (a, b) in enumerate(zip(given, into))]
    for copy in copies:
        copy.start()
    for copy in copies:
        copy.wait()
    points, potential, weight, column_points, column_potential, column_weight, core = into
    value = points[...]
    block = jnp.concatenate([value[8 * k : 8 * k + 8] for k in range(4)], axis=1)
    last = jnp.concatenate(
        [potential[...], weight[...], jnp.ones((1, LANES - 64), F32)], axis=1
    )
    held[0:34, 0:34] = core[...]
    z = lax.axis_index("z")
    share = [held[pl.ds(z + 16 * g, 1), 0:34] for g in range(3)]
    share = jnp.concatenate([*share, jnp.zeros((1, LANES - 3 * 34), F32)], 1)
    both = jnp.concatenate([block, last, share], 0)
    for k in range(out.shape[0] // 10):
        out[10 * k : 10 * k + 10, :] = both
    for r in range(4):
        for k in range(8):
            held[8 * r + k : 8 * r + k + 1, :] = column_points[
                r : r + 1, LANES * k : LANES * k + LANES
            ]
    src = lax.axis_index(("x", "core"))
    held[32:33, :] = column_potential[pl.ds(src, 1), :]
    held[33:34, :] = column_weight[pl.ds(src, 1), :]
    both = held[0:34, :]
    for k in range(column_out.shape[0] // 34):
        column_out[34 * k : 34 * k + 34, :] = both


def column_stack(message, out, offsets, y, log_targets):
    for k in range(8):
        points = jnp.concatenate(
            [message[pl.ds(34 * (4 * s + y) + k, 4, stride=8), :] for s in range(8)], 0
        )
        squares = jnp.sum(points * points, 0, keepdims=True)
        at = 34 * (4 * k + y) + 32
        offset = jnp.log(message[pl.ds(at + 1, 1), :]) - log_targets
        offset = (offset + message[pl.ds(at, 1), :] * (1.0 / EPSILON)) * LOG2E
        offsets[pl.ds(8 * y + k, 1), :] = offset
        tail = jnp.concatenate(
            [squares, jnp.ones((1, LANES), F32), offset, jnp.zeros((5, LANES), F32)], 0
        )
        value = jnp.concatenate([points, tail], 0)
        col = pl.multiple_of(1024 * y + LANES * k, LANES)
        out[:, pl.ds(col, LANES)] = stacked(split(value), LATTER_ORDER)


def in_turns(former, columns, consume, tiles, prepare=None):
    count = len(tiles)
    lead = count // 2
    width = tiles[0].shape[1]
    blocks = columns.shape[1] // width

    def fill(k, b):
        at = pl.multiple_of(jnp.minimum(b, blocks - 1) * width, width)
        tiles[k][...] = dot(former[...], columns[:, pl.ds(at, width)], ((0,), (0,)))

    for k in range(lead):
        fill(k, k)

    def step(i, _):
        for k in range(count):
            if prepare and k == count // 2:
                prepare(i + 1)
            fill((k + lead) % count, count * i + k + lead)
            consume(tiles[k], count * i + k)
        return 0

    lax.fori_loop(0, blocks // count, step, 0)


def signs(core):
    row = lax.broadcasted_iota(jnp.int32, core.shape, 0)
    col = lax.broadcasted_iota(jnp.int32, core.shape, 1)
    core = jnp.where(row < 32, -2.0 * core, core)
    return jnp.where(col < 32, -2.0 * core, core)


def weighted_core(core, features):
    return dot(signs(core), features, ((0,), (0,)), HIGHEST) * (2.0 / EPSILON * LOG2E)


def former_stack(weighted, row_term, column_factor):
    row = lax.broadcasted_iota(jnp.int32, weighted.shape, 0)
    if row_term is not None:
        weighted = jnp.where(row == 33, weighted + row_term * LOG2E, weighted)
    weighted = jnp.where(row == 34, column_factor, weighted)
    return stacked(split(weighted), FORMER_ORDER)


def turned(core):
    core = jnp.concatenate([core[2:34], core[0:2], jnp.zeros((PAD - 34, 34), F32)], 0)
    return jnp.concatenate([core[:, 2:34], core[:, 0:2], jnp.zeros((PAD, PAD - 34), F32)], 1)


def turned_back(core):
    core = jnp.concatenate([core[32:34], core[0:32]], 0)
    return jnp.concatenate([core[:, 32:34], core[:, 0:32]], 1)


def unpacked_sources(message, log_sources):
    pieces = []
    for k in range(4):
        pieces.append(
            jnp.concatenate(
                [message[10 * z : 10 * z + 8, 32 * k : 32 * k + 32] for z in range(16)], 1
            )
        )
    points = jnp.concatenate(pieces, 0)
    last = jnp.concatenate([message[10 * z + 8 : 10 * z + 9, 0:32] for z in range(16)], 1)
    weight = jnp.concatenate([message[10 * z + 8 : 10 * z + 9, 32:64] for z in range(16)], 1)
    squares = jnp.sum(points * points, 0, keepdims=True)
    zeros = jnp.zeros((6, squares.shape[1]), F32)
    features = jnp.concatenate([points, squares, jnp.ones_like(squares), zeros], 0)
    shares = message[pl.ds(9, 16, stride=10), :]
    core = jnp.concatenate([shares[:, 34 * g : 34 * g + 34] for g in range(3)], 0)
    return features, jnp.log(weight) - log_sources, last, turned(core)


def core_to_rows(core):
    tail = jnp.concatenate(
        [core[30:34, 0:26], jnp.concatenate([core[30:34, 26:34], jnp.zeros((4, 18), F32)], 1)], 0
    )
    tail = jnp.concatenate([tail, jnp.zeros((2, 26), F32)], 0)
    groups = [core[10 * g : 10 * g + 10, 0:34] for g in range(3)]
    return jnp.concatenate([*groups, tail], 1)


def core_from_rows(both):
    top = jnp.concatenate([both[:, 34 * g : 34 * g + 34] for g in range(3)], 0)
    last = jnp.concatenate([both[0:4, 102:128], both[4:8, 102:110]], 1)
    core = jnp.concatenate([top, last, jnp.zeros((PAD - 34, 34), F32)], 0)
    return jnp.concatenate([core, jnp.zeros((PAD, PAD - 34), F32)], 1)


def core_kernel(log_sources, log_targets):
    def body(
        message, arrived, packed, columns, features, log_out, offsets, former, total, *tiles
    ):
        value, log_source, potential, core = unpacked_sources(message, log_sources)
        features[...] = value
        log_out[...] = log_source
        former[...] = former_stack(
            weighted_core(core, value), log_source + potential * (1.0 / EPSILON), 1.0
        )
        total[...] = jnp.zeros_like(total)

        def prepare(y):
            column_stack(arrived, columns, offsets, jnp.minimum(y, 3), log_targets)

        prepare(0)

        def consume(tile, b):
            width = tile.shape[1]
            stack = columns[:, pl.ds(pl.multiple_of(b * width, width), width)]
            plan = jnp.exp2(tile[...])
            high = plan.astype(BF16)
            low = (plan - high.astype(F32)).astype(BF16)
            total[...] += dot(high, stack, ((1,), (1,))) + dot(low, stack, ((1,), (1,)))

        in_turns(former, columns, consume, tiles, prepare)
        carried = (
            total[:, 0:PAD] + total[:, 2 * PAD : 3 * PAD] + total[:, 4 * PAD : 5 * PAD]
        )
        part = dot(features[...], carried, ((1,), (0,)), HIGHEST)
        part = jnp.concatenate([part[0:32], part[33:34], part[32:33]], 0)
        part = jnp.concatenate([part[:, 0:32], part[:, 33:34], part[:, 32:33]], 1)
        both = core_to_rows(part)
        for k in range(packed.shape[0] // 10):
            packed[10 * k : 10 * k + 10, :] = both

    return body


def row_kernel(
    parts, features, columns, out, core_out, shares, top_out, former, highest, scores
):
    core = core_from_rows(sum(parts[10 * k : 10 * k + 10, :] for k in range(parts.shape[0] // 10)))
    core_out[...] = core
    former[...] = former_stack(weighted_core(core, features[...]), None, 1.0)
    rows = features.shape[1]
    highest[...] = jnp.full(highest.shape, -jnp.inf, F32)

    def fill(b, _):
        at = pl.ds(pl.multiple_of(2048 * b, 2048), 2048)
        tile = dot(former[...], columns[:, at], ((0,), (0,)))
        scores[:, at] = tile
        pieces = [tile[:, LANES * k : LANES * k + LANES] for k in range(16)]
        highest[...] = largest([highest[...], *pieces])
        return 0

    lax.fori_loop(0, columns.shape[1] // 2048, fill, 0)
    top = jnp.max(highest[...], 1, keepdims=True)
    highest[...] = jnp.broadcast_to(top, highest.shape)

    added = []
    for r in range(0, rows, 8):
        of = pl.ds(r, 8)
        shift = highest[of, :]
        sums = [jnp.zeros((8, LANES), F32) for _ in range(4)]
        for k in range(columns.shape[1] // LANES):
            at = pl.ds(LANES * k, LANES)
            share = jnp.exp2(scores[of, at] - shift)
            shares[of, at] = share
            sums[k % 4] = sums[k % 4] + share
        added.append(sum(sums))
    total = jnp.concatenate(added, 0)
    part = top * LN2 + jnp.log(jnp.sum(total, 1, keepdims=True))
    both = across(jnp.broadcast_to(part, (rows, LANES)))
    for k in range(out.shape[0] // 4):
        out[4 * k : 4 * k + 4, :] = both
    top_out[...] = across(highest)


def across(wide):
    flat = [jnp.transpose(wide[LANES * k : LANES * k + LANES, :])[0:1] for k in range(4)]
    return jnp.concatenate(flat, 0)


def largest(values):
    return functools.reduce(jnp.maximum, values)


def combined(values):
    highest = largest(values)
    total = sum(jnp.exp(v - highest) for v in values)
    return highest + jnp.log(total)


def column_pieces(tile, b):
    count = tile.shape[1] // LANES
    return [(pl.ds(b * count + k, 1), tile[:, LANES * k : LANES * k + LANES]) for k in range(count)]


def in_lanes(rows):
    return jnp.concatenate([rows[k : k + 1] for k in range(rows.shape[0])], 1)


def column_kernel(log_sources):
    def body(
        parts,
        top,
        shares,
        offsets,
        log_source,
        features,
        core,
        columns,
        own_out,
        out,
        former,
        sums,
        held,
        weights,
        mine,
        *tiles,
    ):
        merged = combined([parts[4 * k : 4 * k + 4, :] for k in range(parts.shape[0] // 4)])
        merged = in_lanes(merged)
        logs = log_source[...]
        source_new = EPSILON * (logs - merged)
        own = own_out.shape[1]
        for k in range(mine.shape[0]):
            mine[k : k + 1, :] = source_new[:, own * k : own * k + own]
        own_out[...] = mine[pl.ds(lax.axis_index("z"), 1), :]

        lift = 2.0 * log_sources + LIFT
        term = logs + source_new * (1.0 / EPSILON)
        weight = jnp.exp(term + (in_lanes(top[...]) * LN2 + lift))
        for k in range(4):
            wide = jnp.broadcast_to(weight[:, LANES * k : LANES * k + LANES], (LANES, LANES))
            weights[LANES * k : LANES * k + LANES, :] = jnp.transpose(wide)
        rows = weights.shape[0]

        for b in range(0, shares.shape[1] // LANES, 4):
            totals = [jnp.zeros((8, LANES), F32) for _ in range(4)]
            for r in range(0, rows, 8):
                factor = weights[r : r + 8, :]
                for k in range(4):
                    at = pl.ds(LANES * (b + k), LANES)
                    totals[k] = totals[k] + shares[r : r + 8, at] * factor
            for k in range(4):
                sums[b + k : b + k + 1, :] = jnp.sum(totals[k], 0, keepdims=True)

        held[...] = jnp.log(sums[...]) - offsets[...] * LN2 - lift
        safe = jnp.min(sums[...]) >= FLOOR

        @pl.when(jnp.logical_not(safe))
        def _():
            former[...] = former_stack(weighted_core(core[...], features[...]), term, 0.0)

            def consume(tile, b):
                for at, piece in column_pieces(tile, b):
                    highest = jnp.max(piece, 0, keepdims=True)
                    total = jnp.sum(jnp.exp2(piece - highest), 0, keepdims=True)
                    held[at, :] = highest * LN2 + jnp.log(total)

            in_turns(former, columns, consume, tiles)

        for y in range(4):
            piece = held[8 * y : 8 * y + 8, :]
            for s in range(8):
                at = 8 * (4 * s + y)
                out[at : at + 8, :] = piece

    return body


def last_kernel(log_targets):
    def body(parts, weight, own_rows, core, out, own_out, core_out):
        own_out[...] = own_rows[...]
        core_out[...] = turned_back(core[...])
        merged = combined([parts[8 * k : 8 * k + 8, :] for k in range(parts.shape[0] // 8)])
        out[...] = EPSILON * (jnp.log(weight[...]) - log_targets - merged)

    return body


def on_device(
    source_points,
    target_points,
    source_potential,
    target_potential,
    source_weight,
    target_weight,
    core_previous,
):
    emb, own = source_points.shape
    dims, span = target_points.shape
    n_z, n_y, n_src = lax.axis_size("z"), lax.axis_size("y"), lax.axis_size(("x", "core"))
    n_plane = n_src * n_y
    rows, columns = own * n_z, span * n_y
    log_sources = math.log(own * n_z * n_plane)
    log_targets = math.log(span * n_z * n_y)
    given = (
        source_points,
        source_potential.reshape(1, own),
        source_weight.reshape(1, own),
        target_points,
        target_potential.reshape(8, LANES),
        target_weight.reshape(8, LANES),
        core_previous,
    )
    mine, theirs = pl.pallas_call(
        pack,
        out_shape=(
            pltpu.VMEM((10 * n_z, LANES), F32),
            pltpu.VMEM((34 * n_plane, LANES), F32),
        ),
        in_specs=[pl.BlockSpec(memory_space=pltpu.HBM)] * len(given),
        out_specs=(VMEM, VMEM),
        scratch_shapes=[
            pltpu.VMEM((48, LANES), F32),
            pltpu.SemaphoreType.DMA((len(given),)),
            *(pltpu.VMEM(a.shape, F32) for a in given),
        ],
        compiler_params=pltpu.CompilerParams(vmem_limit_bytes=16 * 2**20),
        name="pack",
    )(*(pltpu.with_memory_space_constraint(a, pltpu.HBM) for a in given))
    theirs = exchange(theirs.reshape(n_plane, 1, 34 * LANES), PLANE).reshape(-1, LANES)
    mine = exchange(mine.reshape(n_z, 1, 10 * LANES), "z").reshape(-1, LANES)
    former = pltpu.VMEM((DEPTH, rows), BF16)
    tile = pltpu.VMEM((rows, 512), F32)
    per_column = (columns // LANES, LANES)
    packed, stack, features, log_source, offsets = call(
        core_kernel(log_sources, log_targets),
        [
            ((10 * n_plane, LANES), F32),
            ((DEPTH, columns), BF16),
            ((PAD, rows), F32),
            ((1, rows), F32),
            (per_column, F32),
        ],
        (mine, theirs),
        scratch=[former, pltpu.VMEM((rows, DEPTH), F32), tile, tile],
        name="core",
        grant=16,
    )
    parts = exchange(packed.reshape(n_plane, 1, 10 * LANES), PLANE)
    parts = jnp.broadcast_to(jnp.sum(parts, 0, keepdims=True), (n_z, 1, 10 * LANES))
    parts = exchange(parts, "z").reshape(-1, LANES)

    per_lane = pltpu.VMEM((rows, LANES), F32)
    row_parts, core, shares, top = call(
        row_kernel,
        [
            ((4 * n_z, LANES), F32),
            ((PAD, PAD), F32),
            ((rows, columns), F32),
            ((rows // LANES, LANES), F32),
        ],
        (parts, features, stack),
        scratch=[former, per_lane, pltpu.VMEM((rows, columns), F32)],
        name="rows",
        grant=24,
    )
    row_parts = exchange(row_parts.reshape(n_z, 1, rows), "z").reshape(-1, LANES)
    own_rows, column_parts = call(
        column_kernel(log_sources),
        [((1, own), F32), ((8 * n_plane, LANES), F32)],
        (row_parts, top, shares, offsets, log_source, features, core, stack),
        scratch=[
            former,
            pltpu.VMEM(per_column, F32),
            pltpu.VMEM(per_column, F32),
            per_lane,
            pltpu.VMEM((n_z, own), F32),
            tile,
            tile,
        ],
        name="columns",
        grant=16,
    )
    column_parts = exchange(column_parts.reshape(n_plane, 1, span), PLANE).reshape(-1, LANES)
    target_new, own_rows, core_new = call(
        last_kernel(log_targets),
        [((8, LANES), F32), ((1, own), F32), (core_previous.shape, F32)],
        (column_parts, target_weight.reshape(8, LANES), own_rows, core),
        name="last",
    )
    return (own_rows.reshape(own), target_new.reshape(span), core_new)


def solution(mesh):
    finer = Mesh(mesh.devices.reshape(4, 2, 4, 16), ALL)
    source, target = P(ALL), P(("y", "z"))
    placed = (
        P(None, ALL),
        P(("x", "core"), ("y", "z")),
        source,
        target,
        source,
        target,
        P(),
    )
    return jax.shard_map(
        on_device, mesh=finer, in_specs=placed, out_specs=(source, target, P()), check_vma=False
    )
```

```python
import functools
import math

import jax
import jax.numpy as jnp
from jax import lax
from jax.experimental import pallas as pl
from jax.experimental.pallas import tpu as pltpu
from jax.sharding import Mesh
from jax.sharding import PartitionSpec as P

PLANE = ("x", "core", "y")
ALL = ("x", "core", "y", "z")
EPSILON = 0.5
HIGHEST = lax.Precision.HIGHEST
LANES = 128
PAD = 40
DEPTH = 256
LOG2E = math.log2(math.e)
LN2 = math.log(2.0)
FLOOR = 2.0**-70
LIFT = 12.0
F32, BF16 = jnp.float32, jnp.bfloat16
VMEM = pl.BlockSpec(memory_space=pltpu.VMEM)


def call(body, outs, args, scratch=(), name=None, grant=8):
    return pl.pallas_call(
        body,
        out_shape=tuple(jax.ShapeDtypeStruct(s, d) for s, d in outs),
        in_specs=[VMEM] * len(args),
        out_specs=tuple(VMEM for _ in outs),
        scratch_shapes=list(scratch),
        compiler_params=pltpu.CompilerParams(vmem_limit_bytes=grant * 2**20),
        name=name,
    )(*args)


def exchange(copies, axis):
    return lax.all_to_all(copies, axis, split_axis=0, concat_axis=0, tiled=True)


def dot(former, latter, dims, precision=None):
    return lax.dot_general(
        former, latter, (dims, ((), ())), precision=precision, preferred_element_type=F32
    )


def split(value):
    first = value.astype(BF16).astype(F32)
    rest = value - first
    second = rest.astype(BF16).astype(F32)
    return first, second, rest - second


def stacked(pieces, order):
    blocks = [pieces[k] for k in order]
    filler = jnp.zeros((DEPTH - PAD * len(order), pieces[0].shape[1]), F32)
    return jnp.concatenate([*blocks, filler], 0).astype(BF16)


LATTER_ORDER = (0, 1, 2, 0, 0, 1)
FORMER_ORDER = (0, 0, 0, 1, 2, 1)


def pack(*refs):
    given, (out, column_out), (held, sem, *into) = refs[:7], refs[7:9], refs[9:]
    copies = [pltpu.make_async_copy(a, b, sem.at[k]) for k, (a, b) in enumerate(zip(given, into))]
    for copy in copies:
        copy.start()
    for copy in copies:
        copy.wait()
    points, potential, weight, column_points, column_potential, column_weight, core = into
    value = points[...]
    block = jnp.concatenate([value[8 * k : 8 * k + 8] for k in range(4)], axis=1)
    last = jnp.concatenate(
        [potential[...], weight[...], jnp.ones((1, LANES - 64), F32)], axis=1
    )
    held[0:34, 0:34] = core[...]
    z = lax.axis_index("z")
    share = [held[pl.ds(z + 16 * g, 1), 0:34] for g in range(3)]
    share = jnp.concatenate([*share, jnp.zeros((1, LANES - 3 * 34), F32)], 1)
    both = jnp.concatenate([block, last, share], 0)
    for k in range(out.shape[0] // 10):
        out[10 * k : 10 * k + 10, :] = both
    for r in range(4):
        for k in range(8):
            held[8 * r + k : 8 * r + k + 1, :] = column_points[
                r : r + 1, LANES * k : LANES * k + LANES
            ]
    src = lax.axis_index(("x", "core"))
    held[32:33, :] = column_potential[pl.ds(src, 1), :]
    held[33:34, :] = column_weight[pl.ds(src, 1), :]
    both = held[0:34, :]
    for k in range(column_out.shape[0] // 34):
        column_out[34 * k : 34 * k + 34, :] = both


def column_stack(message, out, offsets, y, log_targets):
    for k in range(8):
        points = jnp.concatenate(
            [message[pl.ds(34 * (4 * s + y) + k, 4, stride=8), :] for s in range(8)], 0
        )
        squares = jnp.sum(points * points, 0, keepdims=True)
        at = 34 * (4 * k + y) + 32
        offset = jnp.log(message[pl.ds(at + 1, 1), :]) - log_targets
        offset = (offset + message[pl.ds(at, 1), :] * (1.0 / EPSILON)) * LOG2E
        offsets[pl.ds(8 * y + k, 1), :] = offset
        tail = jnp.concatenate(
            [squares, jnp.ones((1, LANES), F32), offset, jnp.zeros((5, LANES), F32)], 0
        )
        value = jnp.concatenate([points, tail], 0)
        col = pl.multiple_of(1024 * y + LANES * k, LANES)
        out[:, pl.ds(col, LANES)] = stacked(split(value), LATTER_ORDER)


def in_turns(former, columns, consume, tiles, prepare=None):
    count = len(tiles)
    lead = count // 2
    width = tiles[0].shape[1]
    blocks = columns.shape[1] // width

    def fill(k, b):
        at = pl.multiple_of(jnp.minimum(b, blocks - 1) * width, width)
        tiles[k][...] = dot(former[...], columns[:, pl.ds(at, width)], ((0,), (0,)))

    for k in range(lead):
        fill(k, k)

    def step(i, _):
        for k in range(count):
            if prepare and k == count // 2:
                prepare(i + 1)
            fill((k + lead) % count, count * i + k + lead)
            consume(tiles[k], count * i + k)
        return 0

    lax.fori_loop(0, blocks // count, step, 0)


def signs(core):
    row = lax.broadcasted_iota(jnp.int32, core.shape, 0)
    col = lax.broadcasted_iota(jnp.int32, core.shape, 1)
    core = jnp.where(row < 32, -2.0 * core, core)
    return jnp.where(col < 32, -2.0 * core, core)


def weighted_core(core, features):
    return dot(signs(core), features, ((0,), (0,)), HIGHEST) * (2.0 / EPSILON * LOG2E)


def former_stack(weighted, row_term, column_factor):
    row = lax.broadcasted_iota(jnp.int32, weighted.shape, 0)
    if row_term is not None:
        weighted = jnp.where(row == 33, weighted + row_term * LOG2E, weighted)
    weighted = jnp.where(row == 34, column_factor, weighted)
    return stacked(split(weighted), FORMER_ORDER)


def turned(core):
    core = jnp.concatenate([core[2:34], core[0:2], jnp.zeros((PAD - 34, 34), F32)], 0)
    return jnp.concatenate([core[:, 2:34], core[:, 0:2], jnp.zeros((PAD, PAD - 34), F32)], 1)


def turned_back(core):
    core = jnp.concatenate([core[32:34], core[0:32]], 0)
    return jnp.concatenate([core[:, 32:34], core[:, 0:32]], 1)


def unpacked_sources(message, log_sources):
    pieces = []
    for k in range(4):
        pieces.append(
            jnp.concatenate(
                [message[10 * z : 10 * z + 8, 32 * k : 32 * k + 32] for z in range(16)], 1
            )
        )
    points = jnp.concatenate(pieces, 0)
    last = jnp.concatenate([message[10 * z + 8 : 10 * z + 9, 0:32] for z in range(16)], 1)
    weight = jnp.concatenate([message[10 * z + 8 : 10 * z + 9, 32:64] for z in range(16)], 1)
    squares = jnp.sum(points * points, 0, keepdims=True)
    zeros = jnp.zeros((6, squares.shape[1]), F32)
    features = jnp.concatenate([points, squares, jnp.ones_like(squares), zeros], 0)
    shares = message[pl.ds(9, 16, stride=10), :]
    core = jnp.concatenate([shares[:, 34 * g : 34 * g + 34] for g in range(3)], 0)
    return features, jnp.log(weight) - log_sources, last, turned(core)


def core_to_rows(core):
    tail = jnp.concatenate(
        [core[30:34, 0:26], jnp.concatenate([core[30:34, 26:34], jnp.zeros((4, 18), F32)], 1)], 0
    )
    tail = jnp.concatenate([tail, jnp.zeros((2, 26), F32)], 0)
    groups = [core[10 * g : 10 * g + 10, 0:34] for g in range(3)]
    return jnp.concatenate([*groups, tail], 1)


def core_from_rows(both):
    top = jnp.concatenate([both[:, 34 * g : 34 * g + 34] for g in range(3)], 0)
    last = jnp.concatenate([both[0:4, 102:128], both[4:8, 102:110]], 1)
    core = jnp.concatenate([top, last, jnp.zeros((PAD - 34, 34), F32)], 0)
    return jnp.concatenate([core, jnp.zeros((PAD, PAD - 34), F32)], 1)


def core_kernel(log_sources, log_targets):
    def body(
        message, arrived, packed, columns, features, log_out, offsets, former, total, *tiles
    ):
        value, log_source, potential, core = unpacked_sources(message, log_sources)
        features[...] = value
        log_out[...] = log_source
        former[...] = former_stack(
            weighted_core(core, value), log_source + potential * (1.0 / EPSILON), 1.0
        )
        total[...] = jnp.zeros_like(total)

        def prepare(y):
            column_stack(arrived, columns, offsets, jnp.minimum(y, 3), log_targets)

        prepare(0)

        def consume(tile, b):
            width = tile.shape[1]
            stack = columns[0:LANES, pl.ds(pl.multiple_of(b * width, width), width)]
            plan = jnp.exp2(tile[...])
            high = plan.astype(BF16)
            low = (plan - high.astype(F32)).astype(BF16)
            total[...] += dot(high, stack, ((1,), (1,))) + dot(low, stack, ((1,), (1,)))

        in_turns(former, columns, consume, tiles, prepare)
        carried = (
            total[:, 0:PAD] + total[:, PAD : 2 * PAD] + total[:, 2 * PAD : 3 * PAD]
        )
        part = dot(features[...], carried, ((1,), (0,)), HIGHEST)
        part = jnp.concatenate([part[0:32], part[33:34], part[32:33]], 0)
        part = jnp.concatenate([part[:, 0:32], part[:, 33:34], part[:, 32:33]], 1)
        both = core_to_rows(part)
        for k in range(packed.shape[0] // 10):
            packed[10 * k : 10 * k + 10, :] = both

    return body


def row_kernel(
    parts, features, columns, out, core_out, shares, top_out, former, highest, scores
):
    core = core_from_rows(sum(parts[10 * k : 10 * k + 10, :] for k in range(parts.shape[0] // 10)))
    core_out[...] = core
    former[...] = former_stack(weighted_core(core, features[...]), None, 1.0)
    rows = features.shape[1]
    highest[...] = jnp.full(highest.shape, -jnp.inf, F32)

    def fill(b, _):
        at = pl.ds(pl.multiple_of(2048 * b, 2048), 2048)
        tile = dot(former[...], columns[:, at], ((0,), (0,)))
        scores[:, at] = tile
        pieces = [tile[:, LANES * k : LANES * k + LANES] for k in range(16)]
        highest[...] = largest([highest[...], *pieces])
        return 0

    lax.fori_loop(0, columns.shape[1] // 2048, fill, 0)
    top = jnp.max(highest[...], 1, keepdims=True)
    highest[...] = jnp.broadcast_to(top, highest.shape)

    added = []
    for r in range(0, rows, 8):
        of = pl.ds(r, 8)
        shift = highest[of, :]
        sums = [jnp.zeros((8, LANES), F32) for _ in range(4)]
        for k in range(columns.shape[1] // LANES):
            at = pl.ds(LANES * k, LANES)
            share = jnp.exp2(scores[of, at] - shift)
            shares[of, at] = share
            sums[k % 4] = sums[k % 4] + share
        added.append(sum(sums))
    total = jnp.concatenate(added, 0)
    part = top * LN2 + jnp.log(jnp.sum(total, 1, keepdims=True))
    both = across(jnp.broadcast_to(part, (rows, LANES)))
    for k in range(out.shape[0] // 4):
        out[4 * k : 4 * k + 4, :] = both
    top_out[...] = across(highest)


def across(wide):
    flat = [jnp.transpose(wide[LANES * k : LANES * k + LANES, :])[0:1] for k in range(4)]
    return jnp.concatenate(flat, 0)


def largest(values):
    return functools.reduce(jnp.maximum, values)


def combined(values):
    highest = largest(values)
    total = sum(jnp.exp(v - highest) for v in values)
    return highest + jnp.log(total)


def column_pieces(tile, b):
    count = tile.shape[1] // LANES
    return [(pl.ds(b * count + k, 1), tile[:, LANES * k : LANES * k + LANES]) for k in range(count)]


def in_lanes(rows):
    return jnp.concatenate([rows[k : k + 1] for k in range(rows.shape[0])], 1)


def column_kernel(log_sources):
    def body(
        parts,
        top,
        shares,
        offsets,
        log_source,
        features,
        core,
        columns,
        own_out,
        out,
        former,
        sums,
        held,
        weights,
        mine,
        *tiles,
    ):
        merged = combined([parts[4 * k : 4 * k + 4, :] for k in range(parts.shape[0] // 4)])
        merged = in_lanes(merged)
        logs = log_source[...]
        source_new = EPSILON * (logs - merged)
        own = own_out.shape[1]
        for k in range(mine.shape[0]):
            mine[k : k + 1, :] = source_new[:, own * k : own * k + own]
        own_out[...] = mine[pl.ds(lax.axis_index("z"), 1), :]

        lift = 2.0 * log_sources + LIFT
        term = logs + source_new * (1.0 / EPSILON)
        weight = jnp.exp(term + (in_lanes(top[...]) * LN2 + lift))
        for k in range(4):
            wide = jnp.broadcast_to(weight[:, LANES * k : LANES * k + LANES], (LANES, LANES))
            weights[LANES * k : LANES * k + LANES, :] = jnp.transpose(wide)
        rows = weights.shape[0]

        for b in range(0, shares.shape[1] // LANES, 4):
            totals = [jnp.zeros((8, LANES), F32) for _ in range(4)]
            for r in range(0, rows, 8):
                factor = weights[r : r + 8, :]
                for k in range(4):
                    at = pl.ds(LANES * (b + k), LANES)
                    totals[k] = totals[k] + shares[r : r + 8, at] * factor
            for k in range(4):
                sums[b + k : b + k + 1, :] = jnp.sum(totals[k], 0, keepdims=True)

        held[...] = jnp.log(sums[...]) - offsets[...] * LN2 - lift
        safe = jnp.min(sums[...]) >= FLOOR

        @pl.when(jnp.logical_not(safe))
        def _():
            former[...] = former_stack(weighted_core(core[...], features[...]), term, 0.0)

            def consume(tile, b):
                for at, piece in column_pieces(tile, b):
                    highest = jnp.max(piece, 0, keepdims=True)
                    total = jnp.sum(jnp.exp2(piece - highest), 0, keepdims=True)
                    held[at, :] = highest * LN2 + jnp.log(total)

            in_turns(former, columns, consume, tiles)

        for y in range(4):
            piece = held[8 * y : 8 * y + 8, :]
            for s in range(8):
                at = 8 * (4 * s + y)
                out[at : at + 8, :] = piece

    return body


def last_kernel(log_targets):
    def body(parts, weight, own_rows, core, out, own_out, core_out):
        own_out[...] = own_rows[...]
        core_out[...] = turned_back(core[...])
        merged = combined([parts[8 * k : 8 * k + 8, :] for k in range(parts.shape[0] // 8)])
        out[...] = EPSILON * (jnp.log(weight[...]) - log_targets - merged)

    return body


def on_device(
    source_points,
    target_points,
    source_potential,
    target_potential,
    source_weight,
    target_weight,
    core_previous,
):
    emb, own = source_points.shape
    dims, span = target_points.shape
    n_z, n_y, n_src = lax.axis_size("z"), lax.axis_size("y"), lax.axis_size(("x", "core"))
    n_plane = n_src * n_y
    rows, columns = own * n_z, span * n_y
    log_sources = math.log(own * n_z * n_plane)
    log_targets = math.log(span * n_z * n_y)
    given = (
        source_points,
        source_potential.reshape(1, own),
        source_weight.reshape(1, own),
        target_points,
        target_potential.reshape(8, LANES),
        target_weight.reshape(8, LANES),
        core_previous,
    )
    mine, theirs = pl.pallas_call(
        pack,
        out_shape=(
            pltpu.VMEM((10 * n_z, LANES), F32),
            pltpu.VMEM((34 * n_plane, LANES), F32),
        ),
        in_specs=[pl.BlockSpec(memory_space=pltpu.HBM)] * len(given),
        out_specs=(VMEM, VMEM),
        scratch_shapes=[
            pltpu.VMEM((48, LANES), F32),
            pltpu.SemaphoreType.DMA((len(given),)),
            *(pltpu.VMEM(a.shape, F32) for a in given),
        ],
        compiler_params=pltpu.CompilerParams(vmem_limit_bytes=16 * 2**20),
        name="pack",
    )(*(pltpu.with_memory_space_constraint(a, pltpu.HBM) for a in given))
    theirs = exchange(theirs.reshape(n_plane, 1, 34 * LANES), PLANE).reshape(-1, LANES)
    mine = exchange(mine.reshape(n_z, 1, 10 * LANES), "z").reshape(-1, LANES)
    former = pltpu.VMEM((DEPTH, rows), BF16)
    tile = pltpu.VMEM((rows, 512), F32)
    per_column = (columns // LANES, LANES)
    packed, stack, features, log_source, offsets = call(
        core_kernel(log_sources, log_targets),
        [
            ((10 * n_plane, LANES), F32),
            ((DEPTH, columns), BF16),
            ((PAD, rows), F32),
            ((1, rows), F32),
            (per_column, F32),
        ],
        (mine, theirs),
        scratch=[former, pltpu.VMEM((rows, LANES), F32), tile, tile],
        name="core",
        grant=16,
    )
    parts = exchange(packed.reshape(n_plane, 1, 10 * LANES), PLANE)
    parts = jnp.broadcast_to(jnp.sum(parts, 0, keepdims=True), (n_z, 1, 10 * LANES))
    parts = exchange(parts, "z").reshape(-1, LANES)

    per_lane = pltpu.VMEM((rows, LANES), F32)
    row_parts, core, shares, top = call(
        row_kernel,
        [
            ((4 * n_z, LANES), F32),
            ((PAD, PAD), F32),
            ((rows, columns), F32),
            ((rows // LANES, LANES), F32),
        ],
        (parts, features, stack),
        scratch=[former, per_lane, pltpu.VMEM((rows, columns), F32)],
        name="rows",
        grant=24,
    )
    row_parts = exchange(row_parts.reshape(n_z, 1, rows), "z").reshape(-1, LANES)
    own_rows, column_parts = call(
        column_kernel(log_sources),
        [((1, own), F32), ((8 * n_plane, LANES), F32)],
        (row_parts, top, shares, offsets, log_source, features, core, stack),
        scratch=[
            former,
            pltpu.VMEM(per_column, F32),
            pltpu.VMEM(per_column, F32),
            per_lane,
            pltpu.VMEM((n_z, own), F32),
            tile,
            tile,
        ],
        name="columns",
        grant=16,
    )
    column_parts = exchange(column_parts.reshape(n_plane, 1, span), PLANE).reshape(-1, LANES)
    target_new, own_rows, core_new = call(
        last_kernel(log_targets),
        [((8, LANES), F32), ((1, own), F32), (core_previous.shape, F32)],
        (column_parts, target_weight.reshape(8, LANES), own_rows, core),
        name="last",
    )
    return (own_rows.reshape(own), target_new.reshape(span), core_new)


def solution(mesh):
    finer = Mesh(mesh.devices.reshape(4, 2, 4, 16), ALL)
    source, target = P(ALL), P(("y", "z"))
    placed = (
        P(None, ALL),
        P(("x", "core"), ("y", "z")),
        source,
        target,
        source,
        target,
        P(),
    )
    return jax.shard_map(
        on_device, mesh=finer, in_specs=placed, out_specs=(source, target, P()), check_vma=False
    )
```
